512 devices in a mesh: dp: 32 (over z, x), mp: 16 (over y, core).
Axes of the slice: x: 4, y: 8, z: 8, core: 2. Of those that a mesh axis runs over, the one named last changes fastest.
Arguments:
- activations: bfloat16 [4096, 4096], P('dp'), may hold values from -6 to 6
- cotangents: bfloat16 [4096, 16384], P('dp', 'mp'), may hold values from -1200 to 1200
- owners: int32 [16], replicated, may hold values from 0 to 31, as said below
Outputs:
- update: bfloat16 [4096, 16384], P('dp', 'mp')
- roots: float32 [16384, 8192], P('dp', 'mp')
- graft: float32 [], replicated
The draws below stay inside these ranges and needn't reach their ends.
Inputs may be any that keep to these rules, and one draw needn't show every extreme that they name: The left root of block b is computed at dp index owners[b] and its right root at owners[b] with its lowest bit flipped; every dp index computes exactly one root.
All inputs are finite; a program needn't handle non-finite values.
Results may differ from the reference program's by a relative error of at most 0.00045.
Values may be sent and summed in bfloat16 or wider, within the bound.
A program may use at most 64 MiB of HBM per device.

```python
import math
import jax
import jax.numpy as jnp
from jax import lax

B = 512
CB = 2
ITERS = 3
RB = 8
NB = 16
DIN = 4096
DOUT = 16384
TOKENS = 4096
N_DP = 32
N_MP = 16


def draw_owners(key, part):
    pair_key = jax.random.fold_in(key, 11)
    side_key = jax.random.fold_in(key, 23)
    pairs = jax.random.permutation(pair_key, NB)
    sides = jax.random.randint(side_key, (NB,), 0, 2)
    return (2 * pairs + sides).astype(jnp.int32)


def draw_cotangents(key, part):
    base_key = jax.random.fold_in(key, 31)
    group_key = jax.random.fold_in(key, 37)
    pick_key = jax.random.fold_in(key, 41)
    base = jax.random.truncated_normal(base_key, -6.0, 6.0, (TOKENS, DOUT), jnp.float32)
    group_ids = jnp.arange(N_MP, dtype=jnp.int32)
    chosen = jax.random.randint(pick_key, (), 0, N_MP)
    group_scale = jnp.exp(jax.random.uniform(group_key, (N_MP,), jnp.float32, jnp.log(0.5), jnp.log(2.0)))
    group_scale = jnp.where(group_ids == chosen, 6.0, group_scale)
    column_scale = jnp.repeat(group_scale, CB * B)
    return (base * column_scale[None, :]).astype(jnp.bfloat16)


def block_levels(rng, dims, split, least, high):
    factor_of = 1.0
    for position, blocks in split:
        draws = jax.random.uniform(jax.random.fold_in(jax.random.fold_in(rng, 6), position), (blocks,), jnp.float32, least / len(split), high / len(split))
        factor_of = factor_of * jnp.repeat(jnp.exp(draws), dims[position] // blocks).reshape((-1,) + (1,) * (len(dims) - 1 - position))
    return factor_of


def normal_values(rng, shape, spread, most, pieces=(), kind=jnp.bfloat16):
    array = spread * jax.random.normal(rng, shape, jnp.float32)
    if pieces:
        array = array * block_levels(rng, shape, pieces, -0.22, 0.18)
    return jnp.clip(array, -most, most).astype(kind)


def setup_inputs(seed: int = 0) -> dict:
    splits = jax.random.split(jax.random.key(seed), 4)
    return {
        "activations": normal_values(splits[0], (TOKENS, DIN), 1.0, 6.0, ((0, 32),)),
        "cotangents": draw_cotangents(jax.random.fold_in(splits[3], 71), 0),
        "owners": draw_owners(jax.random.fold_in(splits[3], 71), 0),
    }


def product(left, right):
    return jnp.dot(left, right, precision=lax.Precision.HIGHEST, preferred_element_type=jnp.float32)

def statistic_of(operand):
    gram = product(operand, operand.T)
    ridge = 0.1 * (jnp.sum(operand * operand) / operand.shape[0] + 1.0)
    return gram + ridge * jnp.eye(operand.shape[0], dtype=jnp.float32)

def inverse_root(statistic):
    eye_matrix = jnp.eye(statistic.shape[0], dtype=jnp.float32)
    magnitude = jnp.sqrt(jnp.sum(statistic * statistic))
    current = statistic / magnitude
    result = eye_matrix
    for step in range(ITERS):
        factor = (5.0 * eye_matrix - current) * 0.25
        if step == 0:
            result = factor * magnitude ** (-0.25)
        else:
            result = product(result, factor)
        if step + 1 < ITERS:
            square = product(factor, factor)
            current = product(product(square, square), current)
    return result

def one_block(grad_block):
    left_root = inverse_root(statistic_of(grad_block))
    right_root = inverse_root(statistic_of(grad_block.T))
    precond = product(left_root, product(grad_block, right_root))
    return (left_root, right_root, precond)

def reference(activations, cotangents, owners):
    gradient = jnp.dot(activations.astype(jnp.float32).T, cotangents.astype(jnp.float32), precision=lax.Precision.HIGHEST, preferred_element_type=jnp.float32) / math.sqrt(TOKENS)
    columns_all = N_MP * CB
    blocks = gradient.reshape(RB, B, columns_all, B).transpose(0, 2, 1, 3).reshape(RB * columns_all, B, B)
    left_all, right_all, precond_all = lax.map(one_block, blocks)
    grad_total = jnp.sum(gradient * gradient)
    precond_total = jnp.sum(precond_all * precond_all)
    graft = jnp.sqrt(grad_total / jnp.maximum(precond_total, 1.0))
    whole = precond_all.reshape(RB, columns_all, B, B).transpose(0, 2, 1, 3).reshape(DIN, DOUT)
    update = (graft * whole).astype(jnp.bfloat16)
    index_dp = jnp.arange(N_DP, dtype=jnp.int32)
    partner = owners + 1 - 2 * (owners % 2)
    left_match = owners[None, :] == index_dp[:, None]
    right_match = partner[None, :] == index_dp[:, None]
    block_ids = jnp.arange(NB, dtype=jnp.int32)
    owned = lax.optimization_barrier(jnp.sum(jnp.where(left_match | right_match, block_ids[None, :], 0), axis=1)).astype(jnp.int32)
    is_left = jnp.any(left_match, axis=1)
    row_block = owned // CB
    col_block = owned % CB
    column_ids = jnp.arange(N_MP, dtype=jnp.int32)[None, :] * CB + col_block[:, None]
    flat_ids = (row_block[:, None] * columns_all + column_ids).astype(jnp.int32)
    picked = jnp.where(is_left[:, None, None, None], left_all[flat_ids], right_all[flat_ids])
    roots = picked.transpose(0, 2, 1, 3).reshape(N_DP * B, N_MP * B)
    return (update, roots, graft)
```

```python
import functools

import jax
import jax.numpy as jnp
from jax import lax
from jax.experimental import pallas as pl
from jax.experimental.pallas import tpu as pltpu
from jax.sharding import Mesh
from jax.sharding import PartitionSpec as P

B = 512
CB = 2
NZ, NX, NY = 8, 4, 8
T = 128
TY = T // NY
MESH_ID = pl.DeviceIdType.MESH
f32, bf16 = jnp.float32, jnp.bfloat16


def gradient_kernel(
    act, cot, g_out, abuf, cbuf, amine, cmine, psend, precv,
    ld_sem, c1_s, c1_r, a1_s, a1_r, a2_s, a2_r, cr_s, cr_r, ar_s, ar_r, p_s, p_r,
):
    z, x, y, c = (lax.axis_index(n) for n in ("z", "x", "y", "c"))
    active = x // 2 == c
    xs = x % 2

    load_c = pltpu.make_async_copy(cot, cmine, ld_sem.at[0])
    load_a = pltpu.make_async_copy(act.at[pl.ds(pl.multiple_of(y * TY, TY), TY), :], amine, ld_sem.at[1])
    load_c.start()
    load_a.start()

    @pl.when(active)
    def _():
        for h in range(2):
            @pl.when(xs == h)
            def _():
                pltpu.make_async_copy(
                    cot.at[:, h * B : (h + 1) * B], cbuf.at[z, xs], c1_r.at[xs]
                ).start()
        pltpu.make_async_copy(
            act.at[pl.ds(pl.multiple_of(y * TY, TY), TY), pl.ds(pl.multiple_of(z * B, B), B)],
            abuf.at[z, xs, y],
            a1_r.at[0],
        ).start()

    bar = pltpu.get_barrier_semaphore()

    def hello(*dev):
        pl.semaphore_signal(bar, inc=1, device_id=dev, device_id_type=MESH_ID)

    for d in range(1, NZ):
        hello((z + d) % NZ, x, y, c)
    for d in range(1, 2 * NX):
        g = (x * 2 + c + d) % (2 * NX)
        hello(z, g // 2, y, g % 2)
    hello(z, x, (y + 1) % NY, c)
    hello(z, x, (y + NY - 1) % NY, c)
    pl.semaphore_wait(bar, NZ - 1 + 2 * NX - 1 + 2)

    load_c.wait()
    load_a.wait()

    def remote(src, dst, s, r, dev):
        return pltpu.make_async_remote_copy(
            src_ref=src, dst_ref=dst, send_sem=s, recv_sem=r, device_id=dev, device_id_type=MESH_ID
        )

    def c1(h):
        return remote(
            cmine.at[:, h * B : (h + 1) * B], cbuf.at[z, xs], c1_s.at[h], c1_r.at[xs], (z, 2 * c + h, y, x // 2)
        )

    for h in range(2):
        @pl.when(2 * c + h != x)
        def _():
            c1(h).start()

    def a1(d):
        zd = (z + d) % NZ
        return remote(
            amine.at[:, pl.ds(pl.multiple_of(zd * B, B), B)], abuf.at[z, xs, y], a1_s.at[d], a1_r.at[d], (zd, x, y, c)
        )

    @pl.when(active)
    def _():
        for d in (4, 3, 5, 2, 6, 1, 7):
            a1(d).start()

    def piece_c(k, o):
        return cbuf.at[k, o]

    def piece_a(k, o):
        return abuf.at[:, (xs + o) % 2, k]

    def ring(piece, pos, n, s_sem, r_sem, dev_of):
        def send(step, o, direction):
            chunk = (pos + n - direction * (step - 1)) % n
            i = (step - 1) * 4 + o * 2 + (direction > 0)
            ref = piece(chunk, o)
            return remote(ref, ref, s_sem.at[i], r_sem.at[i], dev_of((pos + n + direction) % n))

        def arrive(step, o, direction):
            chunk = (pos + n - direction * step) % n
            i = (step - 1) * 4 + o * 2 + (direction > 0)
            ref = piece(chunk, o)
            remote(ref, ref, s_sem.at[i], r_sem.at[i], dev_of((pos + n + direction) % n)).wait_recv()

        return send, arrive

    c_send, c_arrive = ring(piece_c, z, NZ, cr_s, cr_r, lambda k: (k, x, y, c))
    a_send, a_arrive = ring(piece_a, y, NY, ar_s, ar_r, lambda k: (z, x, k, c))
    half = NZ // 2
    moves = [(s, o, d) for s in range(1, half) for o in range(2) for d in (1, -1)] + [(half, 0, 1), (half, 1, -1)]

    for o in range(2):
        c1_wait = remote(cbuf.at[z, o], cbuf.at[z, o], c1_s.at[0], c1_r.at[o], (z, x, y, c))
        c1_wait.wait_recv()
        for d in (1, -1):
            c_send(1, o, d).start()

    def a2(d):
        ref = abuf.at[:, xs, y]
        return remote(ref, ref, a2_s.at[d], a2_r.at[xs], (z, (x + d) % NX, y, c))

    @pl.when(active)
    def _():
        for d in range(NZ):
            ref = abuf.at[(z + NZ - d) % NZ, xs, y]
            remote(ref, ref, a1_s.at[0], a1_r.at[d], (z, x, y, c)).wait_recv()
        for d in (2, 1, 3):
            a2(d).start()

    def a2_wait(s):
        @pl.when(2 * c + s != x)
        def _():
            ref = abuf.at[:, s, y]
            remote(ref, ref, a2_s.at[0], a2_r.at[s], (z, x, y, c)).wait_recv()

    for o in range(2):
        s = (xs + o) % 2
        a2_wait(s)
        for d in (1, -1):
            a_send(1, o, d).start()

    for step in range(2, half + 2):
        for o in range(2):
            for send, arrive in ((c_send, c_arrive), (a_send, a_arrive)):
                for d in (1, -1):
                    if (step - 1, o, d) in moves:
                        arrive(step - 1, o, d)
                    if (step, o, d) in moves:
                        send(step, o, d).start()

    def pcopy(r):
        return remote(psend.at[r], precv.at[r], p_s.at[r], p_r.at[r], (z, x, y, 1 - c))

    rows = B // 4
    cot_all = cbuf[...].reshape(NZ * 2 * T, B)
    for r in range(4):
        lhs = abuf[:, :, :, :, r * rows : (r + 1) * rows].reshape(NZ * 2 * T, rows)
        part = lax.dot_general(lhs, cot_all, (((0,), (0,)), ((), ())), preferred_element_type=f32)
        psend[r] = part * (1.0 / 64.0)
        if r:
            pcopy(r - 1).start()
    pcopy(3).start()

    for h in range(2):
        @pl.when(2 * c + h != x)
        def _():
            c1(h).wait_send()

    @pl.when(active)
    def _():
        for d in range(1, NZ):
            a1(d).wait_send()
        for d in range(1, NX):
            a2(d).wait_send()

    for m in moves:
        c_send(*m).wait_send()
        a_send(*m).wait_send()
    for r in range(4):
        pcopy(r).wait_recv()
        g_out[r * rows : (r + 1) * rows, :] = psend[r] + precv[r]
    for r in range(4):
        pcopy(r).wait_send()


def gradient(act, cot):
    dma = pltpu.SemaphoreType.DMA
    return pl.pallas_call(
        gradient_kernel,
        out_shape=jax.ShapeDtypeStruct((B, B), f32),
        in_specs=[pl.BlockSpec(memory_space=pl.ANY)] * 2,
        out_specs=pl.BlockSpec(memory_space=pltpu.VMEM),
        scratch_shapes=[
            pltpu.VMEM((NZ, 2, NY, TY, B), bf16),
            pltpu.VMEM((NZ, 2, T, B), bf16),
            pltpu.VMEM((TY, NZ * B), bf16),
            pltpu.VMEM((T, CB * B), bf16),
            pltpu.VMEM((4, B // 4, B), f32),
            pltpu.VMEM((4, B // 4, B), f32),
            dma((2,)),
            dma((2,)), dma((2,)),
            dma((NZ,)), dma((NZ,)),
            dma((NX,)), dma((2,)),
            dma((16,)), dma((16,)),
            dma((16,)), dma((16,)),
            dma((4,)), dma((4,)),
        ],
        compiler_params=pltpu.CompilerParams(collective_id=0, has_side_effects=True, vmem_limit_bytes=40 * 2**20),
        name="gradient",
    )(act, cot)


def split(v):
    hi = v.astype(bf16)
    return hi, (v - hi.astype(f32)).astype(bf16)


def dot3(a, b, dims=(((1,), (0,)), ((), ()))):
    def d(p, q):
        return lax.dot_general(p, q, dims, preferred_element_type=f32)

    return d(a[0], b[0]) + (d(a[0], b[1]) + d(a[1], b[0]))


SCALE0 = 1.25**3


def root_kernel(g_ref, d_ref, s_ref, w_ref, v_ref, n_ref, m_ref, r_ref):
    c = lax.axis_index("c")

    def save(ref, v):
        ref[...] = v

    g = g_ref[...]
    ridge = 0.1 * (jnp.sum(g * g, keepdims=True) / B + 1.0)
    eye = (
        lax.broadcasted_iota(jnp.int32, (B, B), 0) == lax.broadcasted_iota(jnp.int32, (B, B), 1)
    )

    @pl.when(c == 0)
    def _():
        gg = split(g_ref[...])
        w_ref[...] = dot3(gg, gg, (((1,), (1,)), ((), ())))

    @pl.when(c == 1)
    def _():
        gg = split(g_ref[...])
        w_ref[...] = dot3(gg, gg, (((0,), (0,)), ((), ())))

    stat = w_ref[...] + jnp.where(eye, ridge, 0.0)
    w_ref[...] = stat
    mag = jnp.sqrt(jnp.sum(stat * stat, keepdims=True))
    s_ref[...] = jnp.broadcast_to(SCALE0 * lax.rsqrt(jnp.sqrt(mag)), s_ref.shape)
    n_ref[...] = w_ref[...] * (0.2 / mag)

    def advance(src, dst):
        n = split(src[...])
        w_ref[...] = dot3(n, n)
        v_ref[...] = dot3(n, split(w_ref[...]))
        u = src[...] - 2.0 * w_ref[...] + v_ref[...]
        v_ref[...] = u
        left = split(w_ref[...] - 2.0 * src[...])
        dst[...] = (1.25**4) * (v_ref[...] + dot3(left, split(v_ref[...])))

    advance(n_ref, m_ref)
    r_ref[...] = n_ref[...] + m_ref[...] - dot3(split(n_ref[...]), split(m_ref[...]))
    advance(m_ref, n_ref)
    d_ref[...] = r_ref[...] + n_ref[...] - dot3(split(r_ref[...]), split(n_ref[...]))


def roots(g):
    return pl.pallas_call(
        root_kernel,
        out_shape=(jax.ShapeDtypeStruct((B, B), f32), jax.ShapeDtypeStruct((8, 128), f32)),
        in_specs=[pl.BlockSpec(memory_space=pltpu.VMEM)],
        out_specs=(pl.BlockSpec(memory_space=pltpu.VMEM),) * 2,
        scratch_shapes=[pltpu.VMEM((B, B), f32)] * 5,
        compiler_params=pltpu.CompilerParams(vmem_limit_bytes=40 * 2**20),
        name="roots",
    )(g)


def product(left, right):
    return jnp.dot(left, right, precision=lax.Precision.HIGHEST, preferred_element_type=f32)


def on_device(act, cot, owners):
    z, x, y, c = (lax.axis_index(n) for n in ("z", "x", "y", "c"))
    g = gradient(act, cot)
    dev, scale = roots(g)
    scale = scale[0, 0]
    eye = jnp.eye(B, dtype=f32)
    q = scale * (eye - dev)
    other = lax.ppermute(q, "c", [(0, 1), (1, 0)])
    left = jnp.where(c == 0, q, other)
    right = jnp.where(c == 0, other, q)
    p = product(left, product(g, right))
    sums = jnp.stack([jnp.sum(g * g, axis=0), jnp.sum(p * p, axis=0)])
    for axis in ("x", "y", "z"):
        sums = lax.psum(sums, axis)
    total = jnp.sum(sums, axis=1)
    graft = jnp.sqrt(total[0] / jnp.maximum(total[1], 1.0))
    out = (graft * p).astype(bf16).reshape(NX, B // NX, B)
    got = lax.all_to_all(out, "x", split_axis=0, concat_axis=0, tiled=True)
    update = jnp.where(c == 0, got[:2], got[2:]).transpose(1, 0, 2).reshape(B // NX, CB * B)

    s0 = scale.astype(bf16)
    s1 = (scale - s0.astype(f32)).astype(bf16)
    s2 = (scale - s0.astype(f32) - s1.astype(f32)).astype(bf16)
    lane = jnp.arange(128)
    extra = jnp.where(lane == 0, s0, jnp.where(lane == 1, s1, jnp.where(lane == 2, s2, jnp.zeros((), bf16))))
    msg = jnp.concatenate([dev.astype(bf16), jnp.broadcast_to(extra[None, :], (B, 128))], axis=1)
    perm = []
    for xx in range(NX):
        for cc in range(2):
            perm.append((xx * 2 + cc, (2 * cc + xx % 2) * 2 + xx // 2))
    msg = lax.ppermute(msg, ("x", "c"), perm)
    msg = lax.all_to_all(msg.reshape(32, 16, 640), ("z", "x"), split_axis=0, concat_axis=0, tiled=True)
    dest = jnp.arange(32, dtype=jnp.int32)
    partner = owners + 1 - 2 * (owners % 2)
    left_match = owners[None, :] == dest[:, None]
    right_match = partner[None, :] == dest[:, None]
    ids = jnp.arange(owners.shape[0], dtype=jnp.int32)
    b = jnp.sum(jnp.where(left_match | right_match, ids[None, :], 0), axis=1)
    side = jnp.where(jnp.any(left_match, axis=1), 0, 1)
    src = (b // 2) * 4 + 2 * side + b % 2
    msg = lax.all_to_all(jnp.take(msg, src, axis=0), ("z", "x"), split_axis=0, concat_axis=0, tiled=True)
    msg = msg.reshape(B, 640)
    mine = jnp.sum(msg[0, B : B + 3].astype(f32))
    root = mine * (eye - msg[:, :B].astype(f32))
    return update, root, graft


def solution(mesh):
    finer = Mesh(mesh.devices.reshape(NZ, NX, NY, 2), ("z", "x", "y", "c"))
    dp, mp = ("z", "x"), ("y", "c")
    return jax.shard_map(
        on_device,
        mesh=finer,
        in_specs=(P(dp, None), P(dp, mp), P()),
        out_specs=(P(dp, mp), P(dp, mp), P()),
        check_vma=False,
    )
```

```python
import functools

import jax
import jax.numpy as jnp
from jax import lax
from jax.experimental import pallas as pl
from jax.experimental.pallas import tpu as pltpu
from jax.sharding import Mesh
from jax.sharding import PartitionSpec as P

B = 512
CB = 2
NZ, NX, NY = 8, 4, 8
T = 128
TY = T // NY
MESH_ID = pl.DeviceIdType.MESH
f32, bf16 = jnp.float32, jnp.bfloat16


def remote(src, dst, s, r, dev):
    return pltpu.make_async_remote_copy(
        src_ref=src, dst_ref=dst, send_sem=s, recv_sem=r, device_id=dev, device_id_type=MESH_ID
    )


def coords():
    return tuple(lax.axis_index(n) for n in ("z", "x", "y", "c"))


def gradient_stage(
    act, cot, g_out, abuf, cbuf, amine, cmine, psend, precv,
    ld_sem, c1_s, c1_r, a1_s, a1_r, a2_s, a2_r, cr_s, cr_r, ar_s, ar_r, p_s, p_r,
):
    z, x, y, c = coords()
    active = x // 2 == c
    xs = x % 2

    load_c = pltpu.make_async_copy(cot, cmine, ld_sem.at[0])
    load_a = pltpu.make_async_copy(act.at[pl.ds(pl.multiple_of(y * TY, TY), TY), :], amine, ld_sem.at[1])
    load_c.start()
    load_a.start()

    @pl.when(active)
    def _():
        for h in range(2):
            @pl.when(xs == h)
            def _():
                pltpu.make_async_copy(
                    cot.at[:, h * B : (h + 1) * B], cbuf.at[z, xs], c1_r.at[xs]
                ).start()
        pltpu.make_async_copy(
            act.at[pl.ds(pl.multiple_of(y * TY, TY), TY), pl.ds(pl.multiple_of(z * B, B), B)],
            abuf.at[z, xs, y],
            a1_r.at[0],
        ).start()

    bar = pltpu.get_barrier_semaphore()

    def hello(*dev):
        pl.semaphore_signal(bar, inc=1, device_id=dev, device_id_type=MESH_ID)

    for d in range(1, 2 * NX * NZ):
        g = (z * 2 * NX + x * 2 + c + d) % (2 * NX * NZ)
        hello(g // (2 * NX), g // 2 % NX, y, g % 2)
    for d in range(1, NY):
        hello(z, x, (y + d) % NY, c)
    pl.semaphore_wait(bar, 2 * NX * NZ - 1 + NY - 1)

    load_c.wait()
    load_a.wait()

    def c1(h):
        return remote(
            cmine.at[:, h * B : (h + 1) * B], cbuf.at[z, xs], c1_s.at[h], c1_r.at[xs], (z, 2 * c + h, y, x // 2)
        )

    for h in range(2):
        @pl.when(2 * c + h != x)
        def _():
            c1(h).start()

    def a1(d):
        zd = (z + d) % NZ
        return remote(
            amine.at[:, pl.ds(pl.multiple_of(zd * B, B), B)], abuf.at[z, xs, y], a1_s.at[d], a1_r.at[d], (zd, x, y, c)
        )

    @pl.when(active)
    def _():
        for d in (4, 3, 5, 2, 6, 1, 7):
            a1(d).start()

    def piece_c(k, o):
        return cbuf.at[k, o]

    def piece_a(k, o):
        return abuf.at[:, (xs + o) % 2, k]

    def ring(piece, pos, n, s_sem, r_sem, dev_of):
        def send(step, o, direction):
            chunk = (pos + n - direction * (step - 1)) % n
            i = (step - 1) * 4 + o * 2 + (direction > 0)
            ref = piece(chunk, o)
            return remote(ref, ref, s_sem.at[i], r_sem.at[i], dev_of((pos + n + direction) % n))

        def arrive(step, o, direction):
            chunk = (pos + n - direction * step) % n
            i = (step - 1) * 4 + o * 2 + (direction > 0)
            ref = piece(chunk, o)
            remote(ref, ref, s_sem.at[i], r_sem.at[i], dev_of((pos + n + direction) % n)).wait_recv()

        return send, arrive

    c_send, c_arrive = ring(piece_c, z, NZ, cr_s, cr_r, lambda k: (k, x, y, c))
    a_send, a_arrive = ring(piece_a, y, NY, ar_s, ar_r, lambda k: (z, x, k, c))
    half = NZ // 2
    moves = [(s, o, d) for s in range(1, half) for o in range(2) for d in (1, -1)] + [(half, 0, 1), (half, 1, -1)]

    for o in range(2):
        c1_wait = remote(cbuf.at[z, o], cbuf.at[z, o], c1_s.at[0], c1_r.at[o], (z, x, y, c))
        c1_wait.wait_recv()
        for d in (1, -1):
            c_send(1, o, d).start()

    def a2(d):
        ref = abuf.at[:, xs, y]
        return remote(ref, ref, a2_s.at[d], a2_r.at[xs], (z, (x + d) % NX, y, c))

    @pl.when(active)
    def _():
        for d in range(NZ):
            ref = abuf.at[(z + NZ - d) % NZ, xs, y]
            remote(ref, ref, a1_s.at[0], a1_r.at[d], (z, x, y, c)).wait_recv()
        for d in (2, 1, 3):
            a2(d).start()

    def a2_wait(s):
        @pl.when(2 * c + s != x)
        def _():
            ref = abuf.at[:, s, y]
            remote(ref, ref, a2_s.at[0], a2_r.at[s], (z, x, y, c)).wait_recv()

    for o in range(2):
        s = (xs + o) % 2
        a2_wait(s)
        for d in (1, -1):
            a_send(1, o, d).start()

    for step in range(2, half + 2):
        for o in range(2):
            for send, arrive in ((c_send, c_arrive), (a_send, a_arrive)):
                for d in (1, -1):
                    if (step - 1, o, d) in moves:
                        arrive(step - 1, o, d)
                    if (step, o, d) in moves:
                        send(step, o, d).start()

    def pcopy(r):
        return remote(psend.at[r], precv.at[r], p_s.at[r], p_r.at[r], (z, x, y, 1 - c))

    rows = B // 4
    cot_all = cbuf[...].reshape(NZ * 2 * T, B)
    for r in range(4):
        lhs = abuf[:, :, :, :, r * rows : (r + 1) * rows].reshape(NZ * 2 * T, rows)
        part = lax.dot_general(lhs, cot_all, (((0,), (0,)), ((), ())), preferred_element_type=f32)
        psend[r] = part * (1.0 / 64.0)
        if r:
            pcopy(r - 1).start()
    pcopy(3).start()

    for h in range(2):
        @pl.when(2 * c + h != x)
        def _():
            c1(h).wait_send()

    @pl.when(active)
    def _():
        for d in range(1, NZ):
            a1(d).wait_send()
        for d in range(1, NX):
            a2(d).wait_send()

    for m in moves:
        c_send(*m).wait_send()
        a_send(*m).wait_send()
    for r in range(4):
        pcopy(r).wait_recv()
        g_out[r * rows : (r + 1) * rows, :] = psend[r] + precv[r]
    for r in range(4):
        pcopy(r).wait_send()


def split(v):
    hi = v.astype(bf16)
    return hi, (v - hi.astype(f32)).astype(bf16)


def dot3(a, b, dims=(((1,), (0,)), ((), ()))):
    def d(p, q):
        return lax.dot_general(p, q, dims, preferred_element_type=f32)

    return d(a[0], b[0]) + (d(a[0], b[1]) + d(a[1], b[0]))


SCALE0 = 1.25**3


def root_stage(g_ref, d_ref, s_ref, w_ref, v_ref, n_ref, m_ref, r_ref):
    c = lax.axis_index("c")

    g = g_ref[...]
    ridge = 0.1 * (jnp.sum(g * g, keepdims=True) / B + 1.0)
    eye = (
        lax.broadcasted_iota(jnp.int32, (B, B), 0) == lax.broadcasted_iota(jnp.int32, (B, B), 1)
    )

    @pl.when(c == 0)
    def _():
        gg = split(g_ref[...])
        w_ref[...] = dot3(gg, gg, (((1,), (1,)), ((), ())))

    @pl.when(c == 1)
    def _():
        gg = split(g_ref[...])
        w_ref[...] = dot3(gg, gg, (((0,), (0,)), ((), ())))

    stat = w_ref[...] + jnp.where(eye, ridge, 0.0)
    w_ref[...] = stat
    mag = jnp.sqrt(jnp.sum(stat * stat, keepdims=True))
    s_ref[...] = jnp.broadcast_to(SCALE0 * lax.rsqrt(jnp.sqrt(mag)), s_ref.shape)
    n_ref[...] = w_ref[...] * (0.2 / mag)

    def advance(src, dst):
        n = split(src[...])
        w_ref[...] = dot3(n, n)
        v_ref[...] = dot3(n, split(w_ref[...]))
        u = src[...] - 2.0 * w_ref[...] + v_ref[...]
        v_ref[...] = u
        left = split(w_ref[...] - 2.0 * src[...])
        dst[...] = (1.25**4) * (v_ref[...] + dot3(left, split(v_ref[...])))

    advance(n_ref, m_ref)
    r_ref[...] = n_ref[...] + m_ref[...] - dot3(split(n_ref[...]), split(m_ref[...]))
    advance(m_ref, n_ref)
    d_ref[...] = r_ref[...] + n_ref[...] - dot3(split(r_ref[...]), split(n_ref[...]))


PAIRS = [(i, j) for i in range(4) for j in range(i, 4)]
MID = 16
PIECE = len(PAIRS) * 128 // MID


def exchange(box, value, me, n, dev_of, s, r):
    box[me] = value
    for d in range(1, n):
        remote(box.at[me], box.at[me], s.at[d], r.at[d], dev_of((me + d) % n)).start()


def exchanged(box, me, n, dev_of, s, r):
    for d in range(1, n):
        ref = box.at[(me + n - d) % n]
        remote(ref, ref, s.at[d], r.at[d], dev_of(me)).wait_recv()
    total = box[0]
    for i in range(1, n):
        total = total + box[i]
    return total


def sent(box, me, n, dev_of, s, r):
    for d in range(1, n):
        remote(box.at[me], box.at[me], s.at[d], r.at[d], dev_of((me + d) % n)).wait_send()


def finish_stage(
    src, g, dev, scale, pbox, bbox, graft,
    dhi, dlo, phi, plo, pscale, pack, abox, stage, t_ref, pout, box1, box2, box3,
    d_s, d_r, a_s, a_r, b_s, b_r, o_s, o_r, e1_s, e1_r, e2_s, e2_r, e3_s, e3_r,
):
    z, x, y, c = coords()
    kappa, xs = x // 2, x % 2
    other = (z, x, y, 1 - c)
    half = B // 2

    dhi[...] = dev[...].astype(bf16)
    dlo[...] = (dev[...] - dhi[...].astype(f32)).astype(bf16)

    for n, (i, j) in enumerate(PAIRS):
        pack[n * 128 : (n + 1) * 128, :] = dhi[i * 128 : (i + 1) * 128, j * 128 : (j + 1) * 128]
    sv = scale[0:1, 0:1]
    s0 = sv.astype(bf16).astype(f32)
    s1 = (sv - s0).astype(bf16).astype(f32)
    s2 = sv - s0 - s1
    row = lax.broadcasted_iota(jnp.int32, (16, 128), 0)
    col = lax.broadcasted_iota(jnp.int32, (16, 128), 1)
    end = pack.shape[0]
    last = pack[end - 16 : end, :].astype(f32)
    for k, v in enumerate((s0, s1, s2)):
        last = jnp.where((row == 15) & (col == k), v, last)
    pack[end - 16 : end, :] = last.astype(bf16)

    def cross(lo):
        rows = pl.ds(lo, B - lo)
        return [
            remote(dhi.at[rows], phi.at[rows], d_s.at[0], d_r.at[0], other),
            remote(dlo.at[rows], plo.at[rows], d_s.at[1], d_r.at[1], other),
            remote(scale, pscale, d_s.at[2], d_r.at[2], other),
        ]

    @pl.when(c == 0)
    def _():
        for t in cross(half):
            t.start()

    @pl.when(c == 1)
    def _():
        for t in cross(0):
            t.start()

    mine = z * 4 + 2 * c + xs
    forwards = xs == c
    k_me = z * 2 + x // 2

    def leg_a(k):
        rows = pl.ds(pl.multiple_of(k * PIECE, 16), PIECE)
        return remote(
            pack.at[rows], abox.at[mine], a_s.at[k], a_r.at[mine], (k // 2, 2 * (k % 2) + kappa, y, kappa)
        )

    def is_me(k):
        return (k == k_me) & forwards & (kappa == c)

    for t in range(MID):
        k = (t + 2 * z) % MID

        @pl.when(jnp.logical_not(is_me(k)))
        def _():
            leg_a(k).start()

    @pl.when(forwards & (kappa == c))
    def _():
        abox[mine] = pack[pl.ds(pl.multiple_of(k_me * PIECE, 16), PIECE), :]

    @pl.when(c == 0)
    def _():
        u = g[:half, :] - dot3((dhi[:half, :], dlo[:half, :]), split(g[...]))
        t_ref[:half, :] = u
        for t in cross(0):
            t.wait_recv()
        factor = scale[0:1, 0:1] * pscale[0:1, 0:1]
        for r in range(2):
            u = t_ref[r * 128 : (r + 1) * 128, :]
            pout[r] = factor * (u - dot3(split(u), (phi[...], plo[...])))

    @pl.when(c == 1)
    def _():
        t_ref[...] = g[...] - dot3(split(g[...]), (dhi[...], dlo[...]))
        for t in cross(half):
            t.wait_recv()
        factor = scale[0:1, 0:1] * pscale[0:1, 0:1]
        tt = split(t_ref[...])
        for r in range(2):
            rows = slice(half + r * 128, half + (r + 1) * 128)
            pout[r] = factor * (t_ref[rows, :] - dot3((phi[rows, :], plo[rows, :]), tt))

    sum_p = jnp.sum(pout[...] * pout[...], axis=0)
    sum_p = jnp.sum(sum_p, keepdims=True)
    sum_g = 0.5 * jnp.sum(g[...] * g[...], keepdims=True)
    row8 = lax.broadcasted_iota(jnp.int32, (8, 128), 0)
    value = jnp.where(row8 == 0, sum_p, jnp.where(row8 == 1, sum_g, 0.0))

    e1 = (box1, x * 2 + c, 2 * NX, lambda i: (z, i // 2, y, i % 2), e1_s, e1_r)
    e2 = (box2, y, NY, lambda i: (z, x, i, c), e2_s, e2_r)
    e3 = (box3, z, NZ, lambda i: (i, x, y, c), e3_s, e3_r)
    exchange(e1[0], value, *e1[1:])

    def rows_to(r):
        return remote(
            pout.at[r], pbox.at[:, pl.ds(pl.multiple_of(xs * B, B), B)], o_s.at[r], o_r.at[xs], (z, 2 * c + r, y, kappa)
        )

    for r in range(2):
        @pl.when(2 * c + r != x)
        def _():
            rows_to(r).start()

        @pl.when(2 * c + r == x)
        def _():
            pbox[:, pl.ds(pl.multiple_of(xs * B, B), B)] = pout[r]

    exchange(e2[0], exchanged(*e1), *e2[1:])

    def leg_b(t):
        d = (z * NX + x + t) % (NZ * NX)
        return remote(stage.at[t], bbox.at[k_me], b_s.at[t], b_r.at[k_me], (d // NX, d % NX, y, c))

    @pl.when(forwards)
    def _():
        for p in range(NZ * NX):
            @pl.when(jnp.logical_not((p == mine) & (kappa == c)))
            def _():
                remote(abox.at[p], abox.at[p], a_s.at[0], a_r.at[p], other).wait_recv()
        for t in range(NZ * NX):
            piece = abox[src[(z * NX + x + t) % (NZ * NX)]]
            if t:
                stage[t] = piece
            else:
                bbox[k_me] = piece
        for t in range(1, NZ * NX):
            leg_b(t).start()

    exchange(e3[0], exchanged(*e2), *e3[1:])
    total = exchanged(*e3)
    graft[...] = jnp.broadcast_to(jnp.sqrt(total[1:2, :] / jnp.maximum(total[0:1, :], 1.0)), graft.shape)

    for s in range(2):
        @pl.when(2 * c + s != x)
        def _():
            ref = pbox.at[:, s * B : (s + 1) * B]
            remote(ref, ref, o_s.at[0], o_r.at[s], other).wait_recv()
    for k in range(MID):
        @pl.when(jnp.logical_not((k == k_me) & forwards))
        def _():
            remote(bbox.at[k], bbox.at[k], b_s.at[0], b_r.at[k], other).wait_recv()

    @pl.when(c == 0)
    def _():
        for t in cross(half):
            t.wait_send()

    @pl.when(c == 1)
    def _():
        for t in cross(0):
            t.wait_send()

    for k in range(MID):
        @pl.when(jnp.logical_not(is_me(k)))
        def _():
            leg_a(k).wait_send()

    for r in range(2):
        @pl.when(2 * c + r != x)
        def _():
            rows_to(r).wait_send()

    @pl.when(forwards)
    def _():
        for t in range(1, NZ * NX):
            leg_b(t).wait_send()

    for e in (e1, e2, e3):
        sent(*e)


N_GRAD = 6 + 13
N_ROOT = 5


def step_kernel(src, act, cot, pbox, bbox, graft, g, dev, scale, *refs):
    grad, root, rest = refs[:N_GRAD], refs[N_GRAD : N_GRAD + N_ROOT], refs[N_GRAD + N_ROOT :]
    gradient_stage(act, cot, g, *grad)
    root_stage(g, dev, scale, *root)
    finish_stage(src, g, dev, scale, pbox, bbox, graft, *rest)


def step(src, act, cot):
    dma = pltpu.SemaphoreType.DMA
    vmem = pltpu.VMEM
    in_vmem = pl.BlockSpec(memory_space=pltpu.VMEM)
    return pl.pallas_call(
        step_kernel,
        out_shape=(
            jax.ShapeDtypeStruct((B // NX, CB * B), f32),
            jax.ShapeDtypeStruct((MID, PIECE, 128), bf16),
            jax.ShapeDtypeStruct((8, 128), f32),
        ),
        in_specs=[
            pl.BlockSpec(memory_space=pltpu.SMEM),
            pl.BlockSpec(memory_space=pl.ANY),
            pl.BlockSpec(memory_space=pl.ANY),
        ],
        out_specs=(in_vmem,) * 3,
        scratch_shapes=[
            vmem((B, B), f32), vmem((B, B), f32), vmem((8, 128), f32),
            vmem((NZ, 2, NY, TY, B), bf16),
            vmem((NZ, 2, T, B), bf16),
            vmem((TY, NZ * B), bf16),
            vmem((T, CB * B), bf16),
            vmem((4, B // 4, B), f32),
            vmem((4, B // 4, B), f32),
            dma((2,)),
            dma((2,)), dma((2,)),
            dma((NZ,)), dma((NZ,)),
            dma((NX,)), dma((2,)),
            dma((16,)), dma((16,)),
            dma((16,)), dma((16,)),
            dma((4,)), dma((4,)),
            *[vmem((B, B), f32)] * N_ROOT,
            vmem((B, B), bf16), vmem((B, B), bf16), vmem((B, B), bf16), vmem((B, B), bf16),
            vmem((8, 128), f32),
            vmem((MID * PIECE, 128), bf16),
            vmem((NZ * NX, PIECE, 128), bf16),
            vmem((NZ * NX, PIECE, 128), bf16),
            vmem((B, B), f32),
            vmem((2, 128, B), f32),
            vmem((8, 8, 128), f32), vmem((8, 8, 128), f32), vmem((8, 8, 128), f32),
            dma((3,)), dma((3,)),
            dma((MID,)), dma((NZ * NX,)),
            dma((NZ * NX,)), dma((MID,)),
            dma((2,)), dma((2,)),
            dma((8,)), dma((8,)), dma((8,)), dma((8,)), dma((8,)), dma((8,)),
        ],
        compiler_params=pltpu.CompilerParams(
            collective_id=0, has_side_effects=True, vmem_limit_bytes=60 * 2**20
        ),
        name="step",
    )(src, act, cot)


def output_kernel(pbox, bbox, graft, update, root):
    update[...] = (graft[0:1, 0:1] * pbox[...]).astype(bf16)
    corner = bbox[len(PAIRS) * 128 - 16 :, :].astype(f32)[15:16, :]
    scale = corner[:, 0:1] + corner[:, 1:2] + corner[:, 2:3]
    row = lax.broadcasted_iota(jnp.int32, (128, 128), 0)
    col = lax.broadcasted_iota(jnp.int32, (128, 128), 1)
    for n, (i, j) in enumerate(PAIRS):
        block = bbox[n * 128 : (n + 1) * 128, :].astype(f32)
        if i == j:
            if i == 3:
                block = jnp.where((row == 127) & (col < 3), block.T, block)
            block = scale * (jnp.where(row == col, 1.0, 0.0) - block)
        else:
            block = -scale * block
            root[j * 128 : (j + 1) * 128, i * 128 : (i + 1) * 128] = block.T
        root[i * 128 : (i + 1) * 128, j * 128 : (j + 1) * 128] = block


def outputs(pbox, bbox, graft):
    vmem = pl.BlockSpec(memory_space=pltpu.VMEM)
    return pl.pallas_call(
        output_kernel,
        out_shape=(jax.ShapeDtypeStruct((B // NX, CB * B), bf16), jax.ShapeDtypeStruct((B, B), f32)),
        in_specs=[vmem] * 3,
        out_specs=(vmem, vmem),
        name="outputs",
    )(pbox, bbox.reshape(MID * PIECE, 128), graft)


def on_device(act, cot, owners):
    dest = jnp.arange(NZ * NX, dtype=jnp.int32)
    left_match = owners[None, :] == dest[:, None]
    right_match = (owners + 1 - 2 * (owners % 2))[None, :] == dest[:, None]
    ids = jnp.arange(owners.shape[0], dtype=jnp.int32)
    place = (ids // 2) * 4 + ids % 2
    src = jnp.sum(jnp.where(left_match, place[None, :], 0) + jnp.where(right_match, place[None, :] + 2, 0), axis=1)
    pbox, bbox, graft = step(src, act, cot)
    update, root = outputs(pbox, bbox, graft)
    return update, root, graft[0, 0]


def solution(mesh):
    finer = Mesh(mesh.devices.reshape(NZ, NX, NY, 2), ("z", "x", "y", "c"))
    dp, mp = ("z", "x"), ("y", "c")
    return jax.shard_map(
        on_device,
        mesh=finer,
        in_specs=(P(dp, None), P(dp, mp), P()),
        out_specs=(P(dp, mp), P(dp, mp), P()),
        check_vma=False,
    )
```

```python
import functools

import jax
import jax.numpy as jnp
from jax import lax
from jax.experimental import pallas as pl
from jax.experimental.pallas import tpu as pltpu
from jax.sharding import Mesh
from jax.sharding import PartitionSpec as P

B = 512
CB = 2
NZ, NX, NY = 8, 4, 8
NB = 16
T = 128
TY = T // NY
MESH_ID = pl.DeviceIdType.MESH
f32, bf16 = jnp.float32, jnp.bfloat16


def remote(src, dst, s, r, dev):
    return pltpu.make_async_remote_copy(
        src_ref=src, dst_ref=dst, send_sem=s, recv_sem=r, device_id=dev, device_id_type=MESH_ID
    )


def coords():
    return tuple(lax.axis_index(n) for n in ("z", "x", "y", "c"))


def gradient_stage(
    act, cot, g_out, table, abuf, cbuf, amine, cmine, psend, precv,
    ld_sem, c1_s, c1_r, a1_s, a1_r, a2_s, a2_r, cr_s, cr_r, ar_s, ar_r, w_s, w_r, p_s, p_r,
):
    z, x, y, c = coords()
    active = x // 2 == c
    xs = x % 2

    load_c = pltpu.make_async_copy(cot, cmine, ld_sem.at[0])
    load_a = pltpu.make_async_copy(act.at[pl.ds(pl.multiple_of(y * TY, TY), TY), :], amine, ld_sem.at[1])
    load_c.start()
    load_a.start()

    @pl.when(active)
    def _():
        for h in range(2):
            @pl.when(xs == h)
            def _():
                pltpu.make_async_copy(
                    cot.at[:, h * B : (h + 1) * B], cbuf.at[z, xs], c1_r.at[xs]
                ).start()
        pltpu.make_async_copy(
            act.at[pl.ds(pl.multiple_of(y * TY, TY), TY), pl.ds(pl.multiple_of(z * B, B), B)],
            abuf.at[z, xs, y],
            a1_r.at[0],
        ).start()

    bar = pltpu.get_barrier_semaphore()

    def hello(*dev):
        pl.semaphore_signal(bar, inc=1, device_id=dev, device_id_type=MESH_ID)

    for d in range(1, 2 * NX * NZ):
        g = (z * 2 * NX + x * 2 + c + d) % (2 * NX * NZ)
        hello(g // (2 * NX), g // 2 % NX, y, g % 2)
    for d in range(1, NY):
        hello(z, x, (y + d) % NY, c)
    pl.semaphore_wait(bar, 2 * NX * NZ - 1 + NY - 1)

    load_c.wait()
    load_a.wait()

    def c1(h):
        return remote(
            cmine.at[:, h * B : (h + 1) * B], cbuf.at[z, xs], c1_s.at[h], c1_r.at[xs], (z, 2 * c + h, y, x // 2)
        )

    for h in range(2):
        @pl.when(2 * c + h != x)
        def _():
            c1(h).start()

    def a1(d):
        zd = (z + d) % NZ
        return remote(
            amine.at[:, pl.ds(pl.multiple_of(zd * B, B), B)], abuf.at[z, xs, y], a1_s, a1_r.at[d], (zd, x, y, c)
        )

    @pl.when(active)
    def _():
        for d in (4, 3, 5, 2, 6, 1, 7):
            a1(d).start()

    table()

    half = NZ // 2
    c_moves = [(s, o, d) for s in range(1, half) for o in range(2) for d in (1, -1)] + [(half, 0, 1), (half, 1, -1)]

    def c_move(step, o, direction, back):
        chunk = (z + NZ - direction * (step - 1 + back)) % NZ
        ref = cbuf.at[chunk, o]
        i = (step - 1) * 4 + o * 2 + (direction > 0)
        return remote(ref, ref, cr_s, cr_r.at[i], ((z + NZ + direction) % NZ, x, y, c))

    def c_step(step):
        for o in range(2):
            for d in (1, -1):
                if (step, o, d) in c_moves:
                    c_move(step, o, d, 1).wait_recv()
                if (step + 1, o, d) in c_moves:
                    c_move(step + 1, o, d, 0).start()

    offsets = (0, -1, 1, -2, 2, -3, 3, 4)
    halves = (slice(0, half), slice(half, NZ))

    def at_y(q):
        return (y + NY + offsets[q]) % NY

    def y_move(step, direction, back):
        k = (y + NY - direction * (step - 1 + back)) % NY
        part = slice(0, NZ) if step < NY // 2 else halves[direction < 0]
        ref = abuf.at[part, xs, k]
        i = (step - 1) * 2 + (direction > 0)
        return remote(ref, ref, ar_s, ar_r.at[i], (z, x, (y + NY + direction) % NY, c))

    def x_move(q, s, direction):
        ref = abuf.at[:, s, at_y(q)]
        i = q * 4 + s * 2 + (direction > 0)
        return remote(ref, ref, a2_s, a2_r.at[i], (z, (x + NX + direction) % NX, y, c))

    def x_half(q, s, direction):
        ref = abuf.at[halves[direction < 0], s, at_y(q)]
        i = q * 4 + s * 2 + (direction > 0)
        return remote(ref, ref, w_s.at[s], w_r.at[i], (z, (x + NX + direction) % NX, y, c))

    def x_start(q):
        for d in (1, -1):
            x_move(q, xs, d).start()

    def x_relay(q):
        for s in range(2):
            for d, place in ((1, 1), (-1, 3)):
                @pl.when((x + NX - 2 * c - s) % NX == place)
                def _():
                    x_move(q, s, d).wait_recv()
                    x_half(q, s, d).start()

    def y_step(step):
        @pl.when(active)
        def _():
            for d in (1, -1):
                y_move(step, d, 1).wait_recv()
                if step + 1 <= NY // 2:
                    y_move(step + 1, d, 0).start()
                if step < NY // 2:
                    x_start(2 * step - (d > 0))
            if step == NY // 2:
                x_start(NY - 1)

    for o in range(2):
        c1_wait = remote(cbuf.at[z, o], cbuf.at[z, o], c1_s.at[0], c1_r.at[o], (z, x, y, c))
        c1_wait.wait_recv()
        for d in (1, -1):
            c_move(1, o, d, 0).start()

    @pl.when(active)
    def _():
        for d in range(NZ):
            ref = abuf.at[(z + NZ - d) % NZ, xs, y]
            remote(ref, ref, a1_s, a1_r.at[d], (z, x, y, c)).wait_recv()
        for d in (1, -1):
            y_move(1, d, 0).start()
        x_start(0)

    y_step(1)
    x_relay(0)
    c_step(1)
    y_step(2)
    x_relay(1)
    x_relay(2)
    y_step(3)
    c_step(2)
    x_relay(3)
    x_relay(4)
    y_step(4)
    x_relay(5)
    x_relay(6)
    c_step(3)
    x_relay(7)
    c_step(4)
    for s in range(2):
        @pl.when((x + NX - 2 * c - s) % NX == 2)
        def _():
            for q in range(NY):
                for d in (1, -1):
                    x_half(q, s, d).wait_recv()

    def pcopy(r):
        return remote(psend.at[r], precv.at[r], p_s.at[r], p_r.at[r], (z, x, y, 1 - c))

    rows = B // 4
    cot_all = cbuf[...].reshape(NZ * 2 * T, B)
    for r in range(4):
        lhs = abuf[:, :, :, :, r * rows : (r + 1) * rows].reshape(NZ * 2 * T, rows)
        part = lax.dot_general(lhs, cot_all, (((0,), (0,)), ((), ())), preferred_element_type=f32)
        psend[r] = part * (1.0 / 64.0)
        if r:
            pcopy(r - 1).start()
    pcopy(3).start()

    for h in range(2):
        @pl.when(2 * c + h != x)
        def _():
            c1(h).wait_send()

    @pl.when(active)
    def _():
        remote(abuf.at[0:7, 0, y], abuf.at[0:7, 0, y], a1_s, a1_r.at[0], (z, x, y, c)).wait_send()
        line = abuf.at[0:7, 0]
        remote(line, line, ar_s, ar_r.at[0], (z, x, y, c)).wait_send()
        line = abuf.at[:, :, :]
        remote(line, line, a2_s, a2_r.at[0], (z, x, y, c)).wait_send()

    for s in range(2):
        @pl.when((x + NX - 2 * c - s) % 2 == 1)
        def _():
            line = abuf.at[0:half, 0]
            remote(line, line, w_s.at[s], w_r.at[0], (z, x, y, c)).wait_send()

    line = cbuf.at[0:7]
    remote(line, line, cr_s, cr_r.at[0], (z, x, y, c)).wait_send()
    for r in range(4):
        pcopy(r).wait_recv()
        g_out[r * rows : (r + 1) * rows, :] = psend[r] + precv[r]
    for r in range(4):
        pcopy(r).wait_send()


def split(v):
    hi = v.astype(bf16)
    return hi, (v - hi.astype(f32)).astype(bf16)


def dot3(a, b, dims=(((1,), (0,)), ((), ()))):
    def d(p, q):
        return lax.dot_general(p, q, dims, preferred_element_type=f32)

    return d(a[0], b[0]) + (d(a[0], b[1]) + d(a[1], b[0]))


def dot1(a, b):
    return jnp.dot(a, b, preferred_element_type=f32)


SCALE0 = 1.25**3


def statistic_stage(g_ref, s_ref, n_ref, w_ref):
    c = lax.axis_index("c")
    g = g_ref[...]
    ridge = 0.1 * (jnp.sum(g * g, keepdims=True) / B + 1.0)
    eye = lax.broadcasted_iota(jnp.int32, (B, B), 0) == lax.broadcasted_iota(jnp.int32, (B, B), 1)

    @pl.when(c == 0)
    def _():
        gg = split(g_ref[...])
        w_ref[...] = dot3(gg, gg, (((1,), (1,)), ((), ())))

    @pl.when(c == 1)
    def _():
        gg = split(g_ref[...])
        w_ref[...] = dot3(gg, gg, (((0,), (0,)), ((), ())))

    stat = w_ref[...] + jnp.where(eye, ridge, 0.0)
    w_ref[...] = stat
    mag = jnp.sqrt(jnp.sum(stat * stat, keepdims=True))
    s_ref[...] = jnp.broadcast_to(SCALE0 * lax.rsqrt(jnp.sqrt(mag)), s_ref.shape)
    n_ref[...] = w_ref[...] * (0.2 / mag)


def chain(n_ref, d_ref, w_ref, v_ref, m_ref, r_ref, parts, dot):
    def advance(src, dst):
        n = parts(src[...])
        w_ref[...] = dot(n, n)
        v_ref[...] = dot(n, parts(w_ref[...]))
        u = src[...] - 2.0 * w_ref[...] + v_ref[...]
        v_ref[...] = u
        left = parts(w_ref[...] - 2.0 * src[...])
        dst[...] = (1.25**4) * (v_ref[...] + dot(left, parts(v_ref[...])))

    advance(n_ref, m_ref)
    r_ref[...] = n_ref[...] + m_ref[...] - dot(parts(n_ref[...]), parts(m_ref[...]))
    advance(m_ref, n_ref)
    d_ref[...] = r_ref[...] + n_ref[...] - dot(parts(r_ref[...]), parts(n_ref[...]))


PAIRS = [(i, j) for i in range(4) for j in range(i, 4)]
MID = 16
PIECE = len(PAIRS) * 128 // MID


def exchange(box, value, me, n, dev_of, s, r):
    box[me] = value
    for d in range(1, n):
        remote(box.at[me], box.at[me], s, r, dev_of((me + d) % n)).start()


def exchanged(box, me, n, dev_of, s, r):
    ref = box.at[0 : n - 1]
    remote(ref, ref, s, r, dev_of(me)).wait_recv()
    total = box[0]
    for i in range(1, n):
        total = total + box[i]
    return total


def sent(box, me, n, dev_of, s, r):
    ref = box.at[0 : n - 1]
    remote(ref, ref, s, r, dev_of(me)).wait_send()


def finish_stage(
    src, g, dev, scale, root_refs, pbox, root, graft,
    bbox, dhi, dlo, phi, plo, pscale, pack, abox, stage, t_ref, pout, box1, box2, box3,
    d_s, d_r, a_s, a_r, b_s, b_r, o_s, o_r, e1_s, e1_r, e2_s, e2_r, e3_s, e3_r,
):
    z, x, y, c = coords()
    kappa, xs = x // 2, x % 2
    other = (z, x, y, 1 - c)
    half = B // 2

    n_ref, w_ref, v_ref, m_ref, r_ref = root_refs
    for n, (i, j) in enumerate(PAIRS):
        pack[n * 128 : (n + 1) * 128, :] = n_ref[i * 128 : (i + 1) * 128, j * 128 : (j + 1) * 128].astype(bf16)
    sv = scale[0:1, 0:1]
    s0 = sv.astype(bf16).astype(f32)
    s1 = (sv - s0).astype(bf16).astype(f32)
    s2 = sv - s0 - s1
    row = lax.broadcasted_iota(jnp.int32, (16, 128), 0)
    col = lax.broadcasted_iota(jnp.int32, (16, 128), 1)
    end = pack.shape[0]
    last = pack[end - 16 : end, :].astype(f32)
    for k, v in enumerate((s0, s1, s2)):
        last = jnp.where((row == 15) & (col == k), v, last)
    pack[end - 16 : end, :] = last.astype(bf16)

    mine = z * 4 + 2 * c + xs
    forwards = xs == c
    k_me = z * 2 + x // 2

    def leg_a(k):
        rows = pl.ds(pl.multiple_of(k * PIECE, 16), PIECE)
        return remote(
            pack.at[rows], abox.at[mine], a_s, a_r, (k // 2, 2 * (k % 2) + kappa, y, kappa)
        )

    def is_me(k):
        return (k == k_me) & forwards & (kappa == c)

    for t in range(MID):
        k = (t + 2 * z) % MID

        @pl.when(jnp.logical_not(is_me(k)))
        def _():
            leg_a(k).start()

    @pl.when(forwards & (kappa == c))
    def _():
        abox[mine] = pack[pl.ds(pl.multiple_of(k_me * PIECE, 16), PIECE), :]

    chain(n_ref, dev, w_ref, v_ref, m_ref, r_ref, split, dot3)
    dhi[...] = dev[...].astype(bf16)
    dlo[...] = (dev[...] - dhi[...].astype(f32)).astype(bf16)

    def cross(lo):
        rows = pl.ds(lo, B - lo)
        return [
            remote(dhi.at[rows], phi.at[rows], d_s.at[0], d_r.at[0], other),
            remote(dlo.at[rows], plo.at[rows], d_s.at[1], d_r.at[1], other),
            remote(scale, pscale, d_s.at[2], d_r.at[2], other),
        ]

    @pl.when(c == 0)
    def _():
        for t in cross(half):
            t.start()

    @pl.when(c == 1)
    def _():
        for t in cross(0):
            t.start()

    @pl.when(c == 0)
    def _():
        t_ref[:half, :] = g[:half, :] - dot3((dhi[:half, :], dlo[:half, :]), split(g[...]))

    @pl.when(c == 1)
    def _():
        t_ref[...] = g[...] - dot3(split(g[...]), (dhi[...], dlo[...]))

    def leg_b(t):
        d = (z * NX + x + t) % (NZ * NX)
        return remote(stage.at[t], bbox.at[k_me], b_s, b_r, (d // NX, d % NX, y, c))

    @pl.when(forwards)
    def _():
        for there in range(2):
            @pl.when((kappa == c) == bool(there))
            def _():
                ref = abox.at[0 : NZ * NX - there]
                remote(ref, ref, a_s, a_r, other).wait_recv()
        for t in range(NZ * NX):
            piece = abox[src[(z * NX + x + t) % (NZ * NX)]]
            if t:
                stage[t] = piece
            else:
                bbox[k_me] = piece
    @pl.when(c == 0)
    def _():
        for t in cross(0):
            t.wait_recv()
        factor = scale[0:1, 0:1] * pscale[0:1, 0:1]
        for r in range(2):
            u = t_ref[r * 128 : (r + 1) * 128, :]
            pout[r] = factor * (u - dot3(split(u), (phi[...], plo[...])))

    @pl.when(c == 1)
    def _():
        for t in cross(half):
            t.wait_recv()
        factor = scale[0:1, 0:1] * pscale[0:1, 0:1]
        tt = split(t_ref[...])
        for r in range(2):
            rows = slice(half + r * 128, half + (r + 1) * 128)
            pout[r] = factor * (t_ref[rows, :] - dot3((phi[rows, :], plo[rows, :]), tt))

    sum_p = jnp.sum(pout[...] * pout[...], axis=0)
    sum_p = jnp.sum(sum_p, keepdims=True)
    sum_g = 0.5 * jnp.sum(g[...] * g[...], keepdims=True)
    row8 = lax.broadcasted_iota(jnp.int32, (8, 128), 0)
    value = jnp.where(row8 == 0, sum_p, jnp.where(row8 == 1, sum_g, 0.0))

    e1 = (box1, x * 2 + c, 2 * NX, lambda i: (z, i // 2, y, i % 2), e1_s, e1_r)
    e2 = (box2, y, NY, lambda i: (z, x, i, c), e2_s, e2_r)
    e3 = (box3, z, NZ, lambda i: (i, x, y, c), e3_s, e3_r)
    exchange(e1[0], value, *e1[1:])

    @pl.when(forwards)
    def _():
        for t in range(1, NZ * NX):
            leg_b(t).start()


    def rows_to(r):
        return remote(
            pout.at[r], pbox.at[:, pl.ds(pl.multiple_of(xs * B, B), B)], o_s.at[r], o_r.at[xs], (z, 2 * c + r, y, kappa)
        )

    for r in range(2):
        @pl.when(2 * c + r != x)
        def _():
            rows_to(r).start()

        @pl.when(2 * c + r == x)
        def _():
            pbox[:, pl.ds(pl.multiple_of(xs * B, B), B)] = pout[r]

    exchange(e2[0], exchanged(*e1), *e2[1:])
    exchange(e3[0], exchanged(*e2), *e3[1:])

    for there in range(2):
        @pl.when(forwards == bool(there))
        def _():
            ref = bbox.at[0 : MID - there]
            remote(ref, ref, b_s, b_r, other).wait_recv()

    row = lax.broadcasted_iota(jnp.int32, (128, 128), 0)
    col = lax.broadcasted_iota(jnp.int32, (128, 128), 1)
    whole = bbox[...].reshape(MID * PIECE, 128)
    for n, (i, j) in enumerate(PAIRS):
        block = whole[n * 128 : (n + 1) * 128, :].astype(f32)
        if i != j:
            n_ref[j * 128 : (j + 1) * 128, i * 128 : (i + 1) * 128] = block.T
        elif i == 3:
            corner = block[127:128, :]
            got = corner[:, 0:1] + corner[:, 1:2] + corner[:, 2:3]
            block = jnp.where((row == 127) & (col < 3), block.T, block)
        n_ref[i * 128 : (i + 1) * 128, j * 128 : (j + 1) * 128] = block
    chain(n_ref, dev, w_ref, v_ref, m_ref, r_ref, lambda v: v.astype(bf16), dot1)
    eye = lax.broadcasted_iota(jnp.int32, (B, B), 0) == lax.broadcasted_iota(jnp.int32, (B, B), 1)
    root[...] = got * (jnp.where(eye, 1.0, 0.0) - dev[...])
    total = exchanged(*e3)
    graft[...] = jnp.broadcast_to(jnp.sqrt(total[1:2, :] / jnp.maximum(total[0:1, :], 1.0)), graft.shape)

    for s in range(2):
        @pl.when(2 * c + s != x)
        def _():
            ref = pbox.at[:, s * B : (s + 1) * B]
            remote(ref, ref, o_s.at[0], o_r.at[s], other).wait_recv()

    @pl.when(c == 0)
    def _():
        for t in cross(half):
            t.wait_send()

    @pl.when(c == 1)
    def _():
        for t in cross(0):
            t.wait_send()

    for there in range(2):
        @pl.when((forwards & (kappa == c)) == bool(there))
        def _():
            ref = pack.at[0 : (MID - there) * PIECE]
            remote(ref, ref, a_s, a_r, other).wait_send()

    for r in range(2):
        @pl.when(2 * c + r != x)
        def _():
            rows_to(r).wait_send()

    @pl.when(forwards)
    def _():
        ref = stage.at[1 : NZ * NX]
        remote(ref, ref, b_s, b_r, other).wait_send()

    for e in (e1, e2, e3):
        sent(*e)


N_GRAD = 6 + 15
N_ROOT = 5


def step_kernel(owners, act, cot, pbox, root, graft, g, dev, scale, own, src, own_sem, *refs):
    grad, spare, rest = refs[:N_GRAD], refs[N_GRAD : N_GRAD + N_ROOT], refs[N_GRAD + N_ROOT :]
    load = pltpu.make_async_copy(owners, own, own_sem)
    load.start()

    def table():
        load.wait()

        def entry(d, carry):
            place = jnp.int32(0)
            for b in range(NB):
                at = (b // 2) * 4 + b % 2
                o = own[b]
                place = jnp.where(o == d, at, place)
                place = jnp.where(o + 1 - 2 * (o % 2) == d, at + 2, place)
            src[d] = place
            return carry

        lax.fori_loop(0, NZ * NX, entry, 0)

    gradient_stage(act, cot, g, table, *grad)
    statistic_stage(g, scale, spare[0], spare[1])
    finish_stage(src, g, dev, scale, spare, pbox, root, graft, *rest)


def step(owners, act, cot):
    dma = pltpu.SemaphoreType.DMA
    vmem = pltpu.VMEM
    in_vmem = pl.BlockSpec(memory_space=pltpu.VMEM)
    return pl.pallas_call(
        step_kernel,
        out_shape=(
            jax.ShapeDtypeStruct((B // NX, CB * B), f32),
            jax.ShapeDtypeStruct((B, B), f32),
            jax.ShapeDtypeStruct((8, 128), f32),
        ),
        in_specs=[pl.BlockSpec(memory_space=pltpu.HBM)] * 3,
        out_specs=(in_vmem,) * 3,
        scratch_shapes=[
            vmem((B, B), f32), vmem((B, B), f32), vmem((8, 128), f32),
            pltpu.SMEM((NB,), jnp.int32), pltpu.SMEM((NZ * NX,), jnp.int32), pltpu.SemaphoreType.DMA,
            vmem((NZ, 2, NY, TY, B), bf16),
            vmem((NZ, 2, T, B), bf16),
            vmem((TY, NZ * B), bf16),
            vmem((T, CB * B), bf16),
            vmem((4, B // 4, B), f32),
            vmem((4, B // 4, B), f32),
            dma((2,)),
            dma((2,)), dma((2,)),
            dma, dma((NZ,)),
            dma, dma((NY * 4,)),
            dma, dma((16,)),
            dma, dma((8,)),
            dma((2,)), dma((NY * 4,)),
            dma((4,)), dma((4,)),
            *[vmem((B, B), f32)] * N_ROOT,
            vmem((MID, PIECE, 128), bf16),
            vmem((B, B), bf16), vmem((B, B), bf16), vmem((B, B), bf16), vmem((B, B), bf16),
            vmem((8, 128), f32),
            vmem((MID * PIECE, 128), bf16),
            vmem((NZ * NX, PIECE, 128), bf16),
            vmem((NZ * NX, PIECE, 128), bf16),
            vmem((B, B), f32),
            vmem((2, 128, B), f32),
            vmem((8, 8, 128), f32), vmem((8, 8, 128), f32), vmem((8, 8, 128), f32),
            dma((3,)), dma((3,)),
            dma, dma, dma, dma,
            dma((2,)), dma((2,)),
            dma, dma, dma, dma, dma, dma,
        ],
        compiler_params=pltpu.CompilerParams(
            collective_id=0, has_side_effects=True, vmem_limit_bytes=52 * 2**20
        ),
        name="step",
    )(owners, act, cot)


def output_kernel(pbox, root_in, graft, update, root, factor, sem):
    copy = pltpu.make_async_copy(root_in, root, sem)
    copy.start()
    update[...] = (graft[0:1, 0:1] * pbox[...]).astype(bf16)
    factor[...] = graft[0:1, 0:1]
    copy.wait()


def outputs(pbox, root, graft):
    vmem = pl.BlockSpec(memory_space=pltpu.VMEM)
    anyw = pl.BlockSpec(memory_space=pl.ANY)
    return pl.pallas_call(
        output_kernel,
        out_shape=(
            jax.ShapeDtypeStruct((B // NX, CB * B), bf16),
            jax.ShapeDtypeStruct((B, B), f32),
            jax.ShapeDtypeStruct((1, 1), f32),
        ),
        in_specs=[vmem, anyw, vmem],
        out_specs=(vmem, anyw, vmem),
        scratch_shapes=[pltpu.SemaphoreType.DMA],
        compiler_params=pltpu.CompilerParams(vmem_limit_bytes=8 * 2**20),
        name="outputs",
    )(pbox, root, graft)


def on_device(act, cot, owners):
    update, root, graft = outputs(*step(owners, act, cot))
    return update, root, graft.reshape(())


def solution(mesh):
    finer = Mesh(mesh.devices.reshape(NZ, NX, NY, 2), ("z", "x", "y", "c"))
    dp, mp = ("z", "x"), ("y", "c")
    return jax.shard_map(
        on_device,
        mesh=finer,
        in_specs=(P(dp, None), P(dp, mp), P()),
        out_specs=(P(dp, mp), P(dp, mp), P()),
        check_vma=False,
    )
```

```python
import functools

import jax
import jax.numpy as jnp
from jax import lax
from jax.experimental import pallas as pl
from jax.experimental.pallas import tpu as pltpu
from jax.sharding import Mesh
from jax.sharding import PartitionSpec as P

B = 512
CB = 2
NZ, NX, NY = 8, 4, 8
NB = 16
T = 128
TY = T // NY
MESH_ID = pl.DeviceIdType.MESH
f32, bf16 = jnp.float32, jnp.bfloat16


def remote(src, dst, s, r, dev):
    return pltpu.make_async_remote_copy(
        src_ref=src, dst_ref=dst, send_sem=s, recv_sem=r, device_id=dev, device_id_type=MESH_ID
    )


def coords():
    return tuple(lax.axis_index(n) for n in ("z", "x", "y", "c"))


def gradient_stage(
    act, cot, g_out, table, abuf, cbuf, amine, cmine, psend, precv,
    ld_sem, c1_s, c1_r, a1_s, a1_r, a2_s, a2_r, cr_s, cr_r, ar_s, ar_r, w_s, w_r, p_s, p_r,
):
    z, x, y, c = coords()
    active = x // 2 == c
    xs = x % 2

    load_c = pltpu.make_async_copy(cot, cmine, ld_sem.at[0])
    load_a = pltpu.make_async_copy(act.at[pl.ds(pl.multiple_of(y * TY, TY), TY), :], amine, ld_sem.at[1])
    load_c.start()
    load_a.start()

    @pl.when(active)
    def _():
        for h in range(2):
            @pl.when(xs == h)
            def _():
                pltpu.make_async_copy(
                    cot.at[:, h * B : (h + 1) * B], cbuf.at[z, xs], c1_r.at[xs]
                ).start()
        pltpu.make_async_copy(
            act.at[pl.ds(pl.multiple_of(y * TY, TY), TY), pl.ds(pl.multiple_of(z * B, B), B)],
            abuf.at[z, xs, y],
            a1_r.at[0],
        ).start()

    bar = pltpu.get_barrier_semaphore()

    def hello(*dev):
        pl.semaphore_signal(bar, inc=1, device_id=dev, device_id_type=MESH_ID)

    for d in range(1, 2 * NX * NZ):
        g = (z * 2 * NX + x * 2 + c + d) % (2 * NX * NZ)
        hello(g // (2 * NX), g // 2 % NX, y, g % 2)
    for d in range(1, NY):
        hello(z, x, (y + d) % NY, c)
    pl.semaphore_wait(bar, 2 * NX * NZ - 1 + NY - 1)

    load_c.wait()
    load_a.wait()

    def c1(h):
        return remote(
            cmine.at[:, h * B : (h + 1) * B], cbuf.at[z, xs], c1_s.at[h], c1_r.at[xs], (z, 2 * c + h, y, x // 2)
        )

    for h in range(2):
        @pl.when(2 * c + h != x)
        def _():
            c1(h).start()

    def a1(d):
        zd = (z + d) % NZ
        return remote(
            amine.at[:, pl.ds(pl.multiple_of(zd * B, B), B)], abuf.at[z, xs, y], a1_s, a1_r.at[d], (zd, x, y, c)
        )

    @pl.when(active)
    def _():
        for d in (4, 3, 5, 2, 6, 1, 7):
            a1(d).start()

    table()

    half = NZ // 2
    c_moves = [(s, o, d) for s in range(1, half) for o in range(2) for d in (1, -1)] + [(half, 0, 1), (half, 1, -1)]

    def c_move(step, o, direction, back):
        chunk = (z + NZ - direction * (step - 1 + back)) % NZ
        ref = cbuf.at[chunk, o]
        i = (step - 1) * 4 + o * 2 + (direction > 0)
        return remote(ref, ref, cr_s, cr_r.at[i], ((z + NZ + direction) % NZ, x, y, c))

    def c_step(step):
        for o in range(2):
            for d in (1, -1):
                if (step, o, d) in c_moves:
                    c_move(step, o, d, 1).wait_recv()
                if (step + 1, o, d) in c_moves:
                    c_move(step + 1, o, d, 0).start()

    offsets = (0, -1, 1, -2, 2, -3, 3, 4)
    halves = (slice(0, half), slice(half, NZ))

    def at_y(q):
        return (y + NY + offsets[q]) % NY

    def y_move(step, direction, back, part):
        k = (y + NY - direction * (step - 1 + back)) % NY
        ref = abuf.at[halves[part], xs, k]
        i = (step - 1) * 4 + part * 2 + (direction > 0)
        return remote(ref, ref, ar_s, ar_r.at[i], (z, x, (y + NY + direction) % NY, c))

    def y_parts(step, direction):
        return (0, 1) if step < NY // 2 else (int(direction < 0),)

    def x_move(q, s, direction):
        ref = abuf.at[:, s, at_y(q)]
        i = q * 4 + s * 2 + (direction > 0)
        return remote(ref, ref, a2_s, a2_r.at[i], (z, (x + NX + direction) % NX, y, c))

    def x_half(q, s, direction):
        ref = abuf.at[halves[direction < 0], s, at_y(q)]
        i = q * 4 + s * 2 + (direction > 0)
        return remote(ref, ref, w_s.at[s], w_r.at[i], (z, (x + NX + direction) % NX, y, c))

    def x_start(q):
        for d in (1, -1):
            x_move(q, xs, d).start()

    def x_relay(q):
        for s in range(2):
            for d, place in ((1, 1), (-1, 3)):
                @pl.when((x + NX - 2 * c - s) % NX == place)
                def _():
                    x_move(q, s, d).wait_recv()
                    x_half(q, s, d).start()

    def y_step(step):
        @pl.when(active)
        def _():
            for part in range(2):
                for d in (1, -1):
                    if part in y_parts(step, d):
                        y_move(step, d, 1, part).wait_recv()
                    if step < NY // 2 and part in y_parts(step + 1, d):
                        y_move(step + 1, d, 0, part).start()
            if step < NY // 2:
                x_start(2 * step - 1)
                x_start(2 * step)
            else:
                x_start(NY - 1)

    for o in range(2):
        c1_wait = remote(cbuf.at[z, o], cbuf.at[z, o], c1_s.at[0], c1_r.at[o], (z, x, y, c))
        c1_wait.wait_recv()
        for d in (1, -1):
            c_move(1, o, d, 0).start()

    @pl.when(active)
    def _():
        for d in range(NZ):
            ref = abuf.at[(z + NZ - d) % NZ, xs, y]
            remote(ref, ref, a1_s, a1_r.at[d], (z, x, y, c)).wait_recv()
        for part in range(2):
            for d in (1, -1):
                y_move(1, d, 0, part).start()
        x_start(0)

    y_step(1)
    x_relay(0)
    c_step(1)
    y_step(2)
    x_relay(1)
    c_step(2)
    x_relay(2)
    y_step(3)
    x_relay(3)
    x_relay(4)
    y_step(4)
    c_step(3)
    x_relay(5)
    x_relay(6)
    x_relay(7)
    c_step(4)
    for s in range(2):
        @pl.when((x + NX - 2 * c - s) % NX == 2)
        def _():
            for q in range(NY):
                for d in (1, -1):
                    x_half(q, s, d).wait_recv()

    def pcopy(r):
        return remote(psend.at[r], precv.at[r], p_s.at[r], p_r.at[r], (z, x, y, 1 - c))

    rows = B // 4
    cot_all = cbuf[...].reshape(NZ * 2 * T, B)
    for r in range(4):
        lhs = abuf[:, :, :, :, r * rows : (r + 1) * rows].reshape(NZ * 2 * T, rows)
        part = lax.dot_general(lhs, cot_all, (((0,), (0,)), ((), ())), preferred_element_type=f32)
        psend[r] = part * (1.0 / 64.0)
        pcopy(r).start()

    for h in range(2):
        @pl.when(2 * c + h != x)
        def _():
            c1(h).wait_send()

    @pl.when(active)
    def _():
        remote(abuf.at[0:7, 0, y], abuf.at[0:7, 0, y], a1_s, a1_r.at[0], (z, x, y, c)).wait_send()
        line = abuf.at[0:7, 0]
        remote(line, line, ar_s, ar_r.at[0], (z, x, y, c)).wait_send()
        line = abuf.at[:, :, :]
        remote(line, line, a2_s, a2_r.at[0], (z, x, y, c)).wait_send()

    for s in range(2):
        @pl.when((x + NX - 2 * c - s) % 2 == 1)
        def _():
            line = abuf.at[0:half, 0]
            remote(line, line, w_s.at[s], w_r.at[0], (z, x, y, c)).wait_send()

    line = cbuf.at[0:7]
    remote(line, line, cr_s, cr_r.at[0], (z, x, y, c)).wait_send()
    for r in range(4):
        pcopy(r).wait_recv()
        g_out[r * rows : (r + 1) * rows, :] = psend[r] + precv[r]
    for r in range(4):
        pcopy(r).wait_send()


def split(v):
    hi = v.astype(bf16)
    return hi, (v - hi.astype(f32)).astype(bf16)


def dot3(a, b, dims=(((1,), (0,)), ((), ()))):
    def d(p, q):
        return lax.dot_general(p, q, dims, preferred_element_type=f32)

    return d(a[0], b[0]) + (d(a[0], b[1]) + d(a[1], b[0]))


def dot1(a, b):
    return jnp.dot(a[0], b[0], preferred_element_type=f32)


def symmetric(ref, top, low):
    half = B // 2
    ref[:half, :] = top
    ref[half:, :half] = top[:, half:].T
    ref[half:, half:] = low


def product_into(ref, a, b, dot):
    half = B // 2
    top = dot([v[:half, :] for v in a], b)
    symmetric(ref, top, dot([v[half:, :] for v in a], [v[:, half:] for v in b]))


SCALE0 = 1.25**3


def statistic_stage(g_ref, s_ref, n_ref, w_ref):
    c = lax.axis_index("c")
    g = g_ref[...]
    ridge = 0.1 * (jnp.sum(g * g, keepdims=True) / B + 1.0)
    eye = lax.broadcasted_iota(jnp.int32, (B, B), 0) == lax.broadcasted_iota(jnp.int32, (B, B), 1)

    half = B // 2

    @pl.when(c == 0)
    def _():
        dims = (((1,), (1,)), ((), ()))
        gg = split(g_ref[...])
        low = [v[half:, :] for v in gg]
        symmetric(w_ref, dot3([v[:half, :] for v in gg], gg, dims), dot3(low, low, dims))

    @pl.when(c == 1)
    def _():
        dims = (((0,), (0,)), ((), ()))
        gg = split(g_ref[...])
        low = [v[:, half:] for v in gg]
        symmetric(w_ref, dot3([v[:, :half] for v in gg], gg, dims), dot3(low, low, dims))

    stat = w_ref[...] + jnp.where(eye, ridge, 0.0)
    w_ref[...] = stat
    mag = jnp.sqrt(jnp.sum(stat * stat, keepdims=True))
    s_ref[...] = jnp.broadcast_to(SCALE0 * lax.rsqrt(jnp.sqrt(mag)), s_ref.shape)
    n_ref[...] = w_ref[...] * (0.2 / mag)


def chain(n_ref, d_ref, w_ref, v_ref, m_ref, r_ref, parts, dot):
    def advance(src, dst):
        n = parts(src[...])
        product_into(w_ref, n, n, dot)
        product_into(v_ref, n, parts(w_ref[...]), dot)
        v_ref[...] = src[...] - 2.0 * w_ref[...] + v_ref[...]
        product_into(dst, parts(w_ref[...] - 2.0 * src[...]), parts(v_ref[...]), dot)
        dst[...] = (1.25**4) * (v_ref[...] + dst[...])

    advance(n_ref, m_ref)
    product_into(r_ref, parts(n_ref[...]), parts(m_ref[...]), dot)
    r_ref[...] = n_ref[...] + m_ref[...] - r_ref[...]
    advance(m_ref, n_ref)
    product_into(d_ref, parts(r_ref[...]), parts(n_ref[...]), dot)
    d_ref[...] = r_ref[...] + n_ref[...] - d_ref[...]


PAIRS = [(i, j) for i in range(4) for j in range(i, 4)]
MID = 16
PIECE = len(PAIRS) * 128 // MID


def exchange(box, value, me, n, dev_of, s, r):
    box[me] = value
    for d in range(1, n):
        remote(box.at[me], box.at[me], s, r, dev_of((me + d) % n)).start()


def exchanged(box, me, n, dev_of, s, r):
    ref = box.at[0 : n - 1]
    remote(ref, ref, s, r, dev_of(me)).wait_recv()
    total = box[0]
    for i in range(1, n):
        total = total + box[i]
    return total


def sent(box, me, n, dev_of, s, r):
    ref = box.at[0 : n - 1]
    remote(ref, ref, s, r, dev_of(me)).wait_send()


def finish_stage(
    src, g, dev, scale, root_refs, pbox, root, graft,
    bbox, dhi, dlo, phi, plo, pscale, pack, abox, stage, t_ref, pout, box1, box2, box3,
    d_s, d_r, a_s, a_r, b_s, b_r, o_s, o_r, e1_s, e1_r, e2_s, e2_r, e3_s, e3_r,
):
    z, x, y, c = coords()
    kappa, xs = x // 2, x % 2
    other = (z, x, y, 1 - c)
    half = B // 2

    n_ref, w_ref, v_ref, m_ref, r_ref = root_refs
    for n, (i, j) in enumerate(PAIRS):
        pack[n * 128 : (n + 1) * 128, :] = n_ref[i * 128 : (i + 1) * 128, j * 128 : (j + 1) * 128].astype(bf16)
    sv = scale[0:1, 0:1]
    s0 = sv.astype(bf16).astype(f32)
    s1 = (sv - s0).astype(bf16).astype(f32)
    s2 = sv - s0 - s1
    row = lax.broadcasted_iota(jnp.int32, (16, 128), 0)
    col = lax.broadcasted_iota(jnp.int32, (16, 128), 1)
    end = pack.shape[0]
    last = pack[end - 16 : end, :].astype(f32)
    for k, v in enumerate((s0, s1, s2)):
        last = jnp.where((row == 15) & (col == k), v, last)
    pack[end - 16 : end, :] = last.astype(bf16)

    mine = z * 4 + 2 * c + xs
    forwards = xs == c
    k_me = z * 2 + x // 2

    def leg_a(k):
        rows = pl.ds(pl.multiple_of(k * PIECE, 16), PIECE)
        return remote(
            pack.at[rows], abox.at[mine], a_s, a_r, (k // 2, 2 * (k % 2) + kappa, y, kappa)
        )

    def is_me(k):
        return (k == k_me) & forwards & (kappa == c)

    far_first = (4, 3, 5, 2, 6, 1, 7, 0)
    for t in range(MID):
        k = (2 * (z + far_first[t // 2]) + t % 2) % MID

        @pl.when(jnp.logical_not(is_me(k)))
        def _():
            leg_a(k).start()

    @pl.when(forwards & (kappa == c))
    def _():
        abox[mine] = pack[pl.ds(pl.multiple_of(k_me * PIECE, 16), PIECE), :]

    chain(n_ref, dev, w_ref, v_ref, m_ref, r_ref, split, dot3)
    dhi[...] = dev[...].astype(bf16)
    dlo[...] = (dev[...] - dhi[...].astype(f32)).astype(bf16)

    def cross(lo):
        rows = pl.ds(lo, B - lo)
        return [
            remote(dhi.at[rows], phi.at[rows], d_s.at[0], d_r.at[0], other),
            remote(dlo.at[rows], plo.at[rows], d_s.at[1], d_r.at[1], other),
            remote(scale, pscale, d_s.at[2], d_r.at[2], other),
        ]

    @pl.when(c == 0)
    def _():
        for t in cross(half):
            t.start()

    @pl.when(c == 1)
    def _():
        for t in cross(0):
            t.start()

    @pl.when(c == 0)
    def _():
        t_ref[:half, :] = g[:half, :] - dot3((dhi[:half, :], dlo[:half, :]), split(g[...]))

    @pl.when(c == 1)
    def _():
        t_ref[...] = g[...] - dot3(split(g[...]), (dhi[...], dlo[...]))

    @pl.when(c == 0)
    def _():
        high, low, scales = cross(0)
        u = t_ref[:half, :]
        uh, ul = split(u)
        high.wait_recv()
        first = jnp.dot(uh, phi[...], preferred_element_type=f32) + jnp.dot(ul, phi[...], preferred_element_type=f32)
        low.wait_recv()
        scales.wait_recv()
        factor = scale[0:1, 0:1] * pscale[0:1, 0:1]
        p = factor * (u - (first + jnp.dot(uh, plo[...], preferred_element_type=f32)))
        pout[0] = p[:128, :]
        pout[1] = p[128:, :]

    @pl.when(c == 1)
    def _():
        for t in cross(half):
            t.wait_recv()
        factor = scale[0:1, 0:1] * pscale[0:1, 0:1]
        tt = split(t_ref[...])
        for r in range(2):
            rows = slice(half + r * 128, half + (r + 1) * 128)
            pout[r] = factor * (t_ref[rows, :] - dot3((phi[rows, :], plo[rows, :]), tt))

    sum_p = jnp.sum(pout[...] * pout[...], axis=0)
    sum_p = jnp.sum(sum_p, keepdims=True)
    sum_g = 0.5 * jnp.sum(g[...] * g[...], keepdims=True)
    row8 = lax.broadcasted_iota(jnp.int32, (8, 128), 0)
    value = jnp.where(row8 == 0, sum_p, jnp.where(row8 == 1, sum_g, 0.0))

    e1 = (box1, x * 2 + c, 2 * NX, lambda i: (z, i // 2, y, i % 2), e1_s, e1_r)
    e2 = (box2, y, NY, lambda i: (z, x, i, c), e2_s, e2_r)
    e3 = (box3, z, NZ, lambda i: (i, x, y, c), e3_s, e3_r)
    exchange(e1[0], value, *e1[1:])


    def rows_to(r):
        return remote(
            pout.at[r], pbox.at[:, pl.ds(pl.multiple_of(xs * B, B), B)], o_s.at[r], o_r.at[xs], (z, 2 * c + r, y, kappa)
        )

    def place_b(t):
        return (z + far_first[t // NX]) % NZ, (x + NX - 1 - t % NX) % NX

    def leg_b(t):
        zd, xd = place_b(t)
        return remote(stage.at[t], bbox.at[k_me], b_s, b_r, (zd, xd, y, c))

    @pl.when(forwards)
    def _():
        for there in range(2):
            @pl.when((kappa == c) == bool(there))
            def _():
                ref = abox.at[0 : NZ * NX - there]
                remote(ref, ref, a_s, a_r, other).wait_recv()
        for t in range(NZ * NX):
            zd, xd = place_b(t)
            piece = abox[src[zd * NX + xd]]
            if t < NZ * NX - 1:
                stage[t] = piece
            else:
                bbox[k_me] = piece
        for t in range(NZ * NX - 1):
            leg_b(t).start()
    for r in range(2):
        @pl.when(2 * c + r != x)
        def _():
            rows_to(r).start()

        @pl.when(2 * c + r == x)
        def _():
            pbox[:, pl.ds(pl.multiple_of(xs * B, B), B)] = pout[r]

    exchange(e2[0], exchanged(*e1), *e2[1:])
    exchange(e3[0], exchanged(*e2), *e3[1:])

    for there in range(2):
        @pl.when(forwards == bool(there))
        def _():
            ref = bbox.at[0 : MID - there]
            remote(ref, ref, b_s, b_r, other).wait_recv()

    row = lax.broadcasted_iota(jnp.int32, (128, 128), 0)
    col = lax.broadcasted_iota(jnp.int32, (128, 128), 1)
    whole = bbox[...].reshape(MID * PIECE, 128)
    for n, (i, j) in enumerate(PAIRS):
        block = whole[n * 128 : (n + 1) * 128, :].astype(f32)
        if i != j:
            n_ref[j * 128 : (j + 1) * 128, i * 128 : (i + 1) * 128] = block.T
        elif i == 3:
            corner = block[127:128, :]
            got = corner[:, 0:1] + corner[:, 1:2] + corner[:, 2:3]
            block = jnp.where((row == 127) & (col < 3), block.T, block)
        n_ref[i * 128 : (i + 1) * 128, j * 128 : (j + 1) * 128] = block
    chain(n_ref, dev, w_ref, v_ref, m_ref, r_ref, lambda v: (v.astype(bf16),), dot1)
    eye = lax.broadcasted_iota(jnp.int32, (B, B), 0) == lax.broadcasted_iota(jnp.int32, (B, B), 1)
    root[...] = got * (jnp.where(eye, 1.0, 0.0) - dev[...])
    total = exchanged(*e3)
    graft[...] = jnp.broadcast_to(jnp.sqrt(total[1:2, :] / jnp.maximum(total[0:1, :], 1.0)), graft.shape)

    for s in range(2):
        @pl.when(2 * c + s != x)
        def _():
            ref = pbox.at[:, s * B : (s + 1) * B]
            remote(ref, ref, o_s.at[0], o_r.at[s], other).wait_recv()

    @pl.when(c == 0)
    def _():
        for t in cross(half):
            t.wait_send()

    @pl.when(c == 1)
    def _():
        for t in cross(0):
            t.wait_send()

    for there in range(2):
        @pl.when((forwards & (kappa == c)) == bool(there))
        def _():
            ref = pack.at[0 : (MID - there) * PIECE]
            remote(ref, ref, a_s, a_r, other).wait_send()

    for r in range(2):
        @pl.when(2 * c + r != x)
        def _():
            rows_to(r).wait_send()

    @pl.when(forwards)
    def _():
        ref = stage.at[0 : NZ * NX - 1]
        remote(ref, ref, b_s, b_r, other).wait_send()

    for e in (e1, e2, e3):
        sent(*e)


N_GRAD = 6 + 15
N_ROOT = 5


def step_kernel(owners, act, cot, pbox, root, graft, g, dev, scale, own, src, own_sem, *refs):
    grad, spare, rest = refs[:N_GRAD], refs[N_GRAD : N_GRAD + N_ROOT], refs[N_GRAD + N_ROOT :]
    load = pltpu.make_async_copy(owners, own, own_sem)
    load.start()

    def table():
        load.wait()

        def entry(d, carry):
            place = jnp.int32(0)
            for b in range(NB):
                at = (b // 2) * 4 + b % 2
                o = own[b]
                place = jnp.where(o == d, at, place)
                place = jnp.where(o + 1 - 2 * (o % 2) == d, at + 2, place)
            src[d] = place
            return carry

        lax.fori_loop(0, NZ * NX, entry, 0)

    gradient_stage(act, cot, g, table, *grad)
    statistic_stage(g, scale, spare[0], spare[1])
    finish_stage(src, g, dev, scale, spare, pbox, root, graft, *rest)


def step(owners, act, cot):
    dma = pltpu.SemaphoreType.DMA
    vmem = pltpu.VMEM
    in_vmem = pl.BlockSpec(memory_space=pltpu.VMEM)
    return pl.pallas_call(
        step_kernel,
        out_shape=(
            jax.ShapeDtypeStruct((B // NX, CB * B), f32),
            jax.ShapeDtypeStruct((B, B), f32),
            jax.ShapeDtypeStruct((8, 128), f32),
        ),
        in_specs=[pl.BlockSpec(memory_space=pltpu.HBM)] * 3,
        out_specs=(in_vmem,) * 3,
        scratch_shapes=[
            vmem((B, B), f32), vmem((B, B), f32), vmem((8, 128), f32),
            pltpu.SMEM((NB,), jnp.int32), pltpu.SMEM((NZ * NX,), jnp.int32), pltpu.SemaphoreType.DMA,
            vmem((NZ, 2, NY, TY, B), bf16),
            vmem((NZ, 2, T, B), bf16),
            vmem((TY, NZ * B), bf16),
            vmem((T, CB * B), bf16),
            vmem((4, B // 4, B), f32),
            vmem((4, B // 4, B), f32),
            dma((2,)),
            dma((2,)), dma((2,)),
            dma, dma((NZ,)),
            dma, dma((NY * 4,)),
            dma, dma((16,)),
            dma, dma((16,)),
            dma((2,)), dma((NY * 4,)),
            dma((4,)), dma((4,)),
            *[vmem((B, B), f32)] * N_ROOT,
            vmem((MID, PIECE, 128), bf16),
            vmem((B, B), bf16), vmem((B, B), bf16), vmem((B, B), bf16), vmem((B, B), bf16),
            vmem((8, 128), f32),
            vmem((MID * PIECE, 128), bf16),
            vmem((NZ * NX, PIECE, 128), bf16),
            vmem((NZ * NX, PIECE, 128), bf16),
            vmem((B, B), f32),
            vmem((2, 128, B), f32),
            vmem((8, 8, 128), f32), vmem((8, 8, 128), f32), vmem((8, 8, 128), f32),
            dma((3,)), dma((3,)),
            dma, dma, dma, dma,
            dma((2,)), dma((2,)),
            dma, dma, dma, dma, dma, dma,
        ],
        compiler_params=pltpu.CompilerParams(
            collective_id=0, has_side_effects=True, vmem_limit_bytes=52 * 2**20
        ),
        name="step",
    )(owners, act, cot)


def output_kernel(pbox, root_in, graft, update, root, factor, sem):
    copy = pltpu.make_async_copy(root_in, root, sem)
    copy.start()
    update[...] = (graft[0:1, 0:1] * pbox[...]).astype(bf16)
    factor[...] = graft[0:1, 0:1]
    copy.wait()


def outputs(pbox, root, graft):
    vmem = pl.BlockSpec(memory_space=pltpu.VMEM)
    anyw = pl.BlockSpec(memory_space=pl.ANY)
    return pl.pallas_call(
        output_kernel,
        out_shape=(
            jax.ShapeDtypeStruct((B // NX, CB * B), bf16),
            jax.ShapeDtypeStruct((B, B), f32),
            jax.ShapeDtypeStruct((1, 1), f32),
        ),
        in_specs=[vmem, anyw, vmem],
        out_specs=(vmem, anyw, vmem),
        scratch_shapes=[pltpu.SemaphoreType.DMA],
        compiler_params=pltpu.CompilerParams(vmem_limit_bytes=8 * 2**20),
        name="outputs",
    )(pbox, root, graft)


def on_device(act, cot, owners):
    update, root, graft = outputs(*step(owners, act, cot))
    return update, root, graft.reshape(())


def solution(mesh):
    finer = Mesh(mesh.devices.reshape(NZ, NX, NY, 2), ("z", "x", "y", "c"))
    dp, mp = ("z", "x"), ("y", "c")
    return jax.shard_map(
        on_device,
        mesh=finer,
        in_specs=(P(dp, None), P(dp, mp), P()),
        out_specs=(P(dp, mp), P(dp, mp), P()),
        check_vma=False,
    )
```

```python
import functools

import jax
import jax.numpy as jnp
from jax import lax
from jax.experimental import pallas as pl
from jax.experimental.pallas import tpu as pltpu
from jax.sharding import Mesh
from jax.sharding import PartitionSpec as P

B = 512
CB = 2
NZ, NX, NY = 8, 4, 8
NB = 16
T = 128
TY = T // NY
MESH_ID = pl.DeviceIdType.MESH
f32, bf16 = jnp.float32, jnp.bfloat16


def remote(src, dst, s, r, dev):
    return pltpu.make_async_remote_copy(
        src_ref=src, dst_ref=dst, send_sem=s, recv_sem=r, device_id=dev, device_id_type=MESH_ID
    )


def coords():
    return tuple(lax.axis_index(n) for n in ("z", "x", "y", "c"))


def gradient_stage(
    act, cot, g_out, table, abuf, cbuf, amine, cmine, psend, precv,
    ld_sem, c1_s, c1_r, a1_s, a1_r, a2_s, a2_r, cr_s, cr_r, ar_s, ar_r, w_s, w_r, p_s, p_r,
):
    z, x, y, c = coords()
    active = x // 2 == c
    xs = x % 2

    load_c = pltpu.make_async_copy(cot, cmine, ld_sem.at[0])
    load_a = pltpu.make_async_copy(act.at[pl.ds(pl.multiple_of(y * TY, TY), TY), :], amine, ld_sem.at[1])
    load_c.start()
    load_a.start()

    @pl.when(active)
    def _():
        for h in range(2):
            @pl.when(xs == h)
            def _():
                pltpu.make_async_copy(
                    cot.at[:, h * B : (h + 1) * B], cbuf.at[z, xs], c1_r.at[xs]
                ).start()
        pltpu.make_async_copy(
            act.at[pl.ds(pl.multiple_of(y * TY, TY), TY), pl.ds(pl.multiple_of(z * B, B), B)],
            abuf.at[z, xs, y],
            a1_r.at[0],
        ).start()

    bar = pltpu.get_barrier_semaphore()

    def hello(*dev):
        pl.semaphore_signal(bar, inc=1, device_id=dev, device_id_type=MESH_ID)

    for d in range(1, 2 * NX * NZ):
        g = (z * 2 * NX + x * 2 + c + d) % (2 * NX * NZ)
        hello(g // (2 * NX), g // 2 % NX, y, g % 2)
    for d in range(1, NY):
        hello(z, x, (y + d) % NY, c)
    pl.semaphore_wait(bar, 2 * NX * NZ - 1 + NY - 1)

    load_c.wait()
    load_a.wait()

    def c1(h):
        return remote(
            cmine.at[:, h * B : (h + 1) * B], cbuf.at[z, xs], c1_s.at[h], c1_r.at[xs], (z, 2 * c + h, y, x // 2)
        )

    for h in range(2):
        @pl.when(2 * c + h != x)
        def _():
            c1(h).start()

    def a1(d):
        zd = (z + d) % NZ
        return remote(
            amine.at[:, pl.ds(pl.multiple_of(zd * B, B), B)], abuf.at[z, xs, y], a1_s, a1_r.at[d], (zd, x, y, c)
        )

    @pl.when(active)
    def _():
        for d in (4, 3, 5, 2, 6, 1, 7):
            a1(d).start()

    table()

    half = NZ // 2
    c_moves = [(s, o, d) for s in range(1, half) for o in range(2) for d in (1, -1)] + [(half, 0, 1), (half, 1, -1)]

    def c_move(step, o, direction, back):
        chunk = (z + NZ - direction * (step - 1 + back)) % NZ
        ref = cbuf.at[chunk, o]
        i = (step - 1) * 4 + o * 2 + (direction > 0)
        return remote(ref, ref, cr_s, cr_r.at[i], ((z + NZ + direction) % NZ, x, y, c))

    def c_step(step):
        for o in range(2):
            for d in (1, -1):
                if (step, o, d) in c_moves:
                    c_move(step, o, d, 1).wait_recv()
                if (step + 1, o, d) in c_moves:
                    c_move(step + 1, o, d, 0).start()

    offsets = (0, -1, 1, -2, 2, -3, 3, 4)
    halves = (slice(0, half), slice(half, NZ))

    def at_y(q):
        return (y + NY + offsets[q]) % NY

    def y_move(step, direction, back, part):
        k = (y + NY - direction * (step - 1 + back)) % NY
        ref = abuf.at[halves[part], xs, k]
        i = (step - 1) * 4 + part * 2 + (direction > 0)
        return remote(ref, ref, ar_s, ar_r.at[i], (z, x, (y + NY + direction) % NY, c))

    def y_parts(step, direction):
        return (0, 1) if step < NY // 2 else (int(direction < 0),)

    def x_move(q, s, direction):
        ref = abuf.at[:, s, at_y(q)]
        i = q * 4 + s * 2 + (direction > 0)
        return remote(ref, ref, a2_s, a2_r.at[i], (z, (x + NX + direction) % NX, y, c))

    def x_half(q, s, direction):
        ref = abuf.at[halves[direction < 0], s, at_y(q)]
        i = q * 4 + s * 2 + (direction > 0)
        return remote(ref, ref, w_s.at[s], w_r.at[i], (z, (x + NX + direction) % NX, y, c))

    def x_start(q):
        for d in (1, -1):
            x_move(q, xs, d).start()

    def x_relay(q):
        for s in range(2):
            for d, place in ((1, 1), (-1, 3)):
                @pl.when((x + NX - 2 * c - s) % NX == place)
                def _():
                    x_move(q, s, d).wait_recv()
                    x_half(q, s, d).start()

    def y_step(step):
        @pl.when(active)
        def _():
            for part in range(2):
                for d in (1, -1):
                    if part in y_parts(step, d):
                        y_move(step, d, 1, part).wait_recv()
                    if step < NY // 2 and part in y_parts(step + 1, d):
                        y_move(step + 1, d, 0, part).start()
            if step < NY // 2:
                x_start(2 * step - 1)
                x_start(2 * step)
            else:
                x_start(NY - 1)

    for o in range(2):
        c1_wait = remote(cbuf.at[z, o], cbuf.at[z, o], c1_s.at[0], c1_r.at[o], (z, x, y, c))
        c1_wait.wait_recv()
        for d in (1, -1):
            c_move(1, o, d, 0).start()

    @pl.when(active)
    def _():
        for d in range(NZ):
            ref = abuf.at[(z + NZ - d) % NZ, xs, y]
            remote(ref, ref, a1_s, a1_r.at[d], (z, x, y, c)).wait_recv()
        for part in range(2):
            for d in (1, -1):
                y_move(1, d, 0, part).start()
        x_start(0)

    y_step(1)
    x_relay(0)
    c_step(1)
    y_step(2)
    x_relay(1)
    y_step(3)
    c_step(2)
    x_relay(2)
    y_step(4)
    x_relay(3)
    x_relay(4)
    c_step(3)
    x_relay(5)
    x_relay(6)
    x_relay(7)
    c_step(4)
    for s in range(2):
        @pl.when((x + NX - 2 * c - s) % NX == 2)
        def _():
            for q in range(NY):
                for d in (1, -1):
                    x_half(q, s, d).wait_recv()

    def pcopy(r):
        return remote(psend.at[r], precv.at[r], p_s.at[r], p_r.at[r], (z, x, y, 1 - c))

    rows = B // 4
    cot_all = cbuf[...].reshape(NZ * 2 * T, B)
    for r in range(4):
        lhs = abuf[:, :, :, :, r * rows : (r + 1) * rows].reshape(NZ * 2 * T, rows)
        part = lax.dot_general(lhs, cot_all, (((0,), (0,)), ((), ())), preferred_element_type=f32)
        psend[r] = part * (1.0 / 64.0)
        pcopy(r).start()

    for h in range(2):
        @pl.when(2 * c + h != x)
        def _():
            c1(h).wait_send()

    @pl.when(active)
    def _():
        remote(abuf.at[0:7, 0, y], abuf.at[0:7, 0, y], a1_s, a1_r.at[0], (z, x, y, c)).wait_send()
        line = abuf.at[0:7, 0]
        remote(line, line, ar_s, ar_r.at[0], (z, x, y, c)).wait_send()
        line = abuf.at[:, :, :]
        remote(line, line, a2_s, a2_r.at[0], (z, x, y, c)).wait_send()

    for s in range(2):
        @pl.when((x + NX - 2 * c - s) % 2 == 1)
        def _():
            line = abuf.at[0:half, 0]
            remote(line, line, w_s.at[s], w_r.at[0], (z, x, y, c)).wait_send()

    line = cbuf.at[0:7]
    remote(line, line, cr_s, cr_r.at[0], (z, x, y, c)).wait_send()
    for r in range(4):
        pcopy(r).wait_recv()
        g_out[r * rows : (r + 1) * rows, :] = psend[r] + precv[r]
    for r in range(4):
        pcopy(r).wait_send()


def split(v):
    hi = v.astype(bf16)
    return hi, (v - hi.astype(f32)).astype(bf16)


def dot3(a, b, dims=(((1,), (0,)), ((), ()))):
    def d(p, q):
        return lax.dot_general(p, q, dims, preferred_element_type=f32)

    return d(a[0], b[0]) + (d(a[0], b[1]) + d(a[1], b[0]))


def dot1(a, b):
    return jnp.dot(a[0], b[0], preferred_element_type=f32)


def symmetric(ref, top, low):
    half = B // 2
    ref[:half, :] = top
    ref[half:, :half] = top[:, half:].T
    ref[half:, half:] = low


def product_into(ref, a, b, dot):
    half = B // 2
    top = dot([v[:half, :] for v in a], b)
    symmetric(ref, top, dot([v[half:, :] for v in a], [v[:, half:] for v in b]))


SCALE0 = 1.25**3


def statistic_stage(g_ref, s_ref, n_ref, w_ref):
    c = lax.axis_index("c")
    g = g_ref[...]
    ridge = 0.1 * (jnp.sum(g * g, keepdims=True) / B + 1.0)
    eye = lax.broadcasted_iota(jnp.int32, (B, B), 0) == lax.broadcasted_iota(jnp.int32, (B, B), 1)

    half = B // 2

    @pl.when(c == 0)
    def _():
        dims = (((1,), (1,)), ((), ()))
        gg = split(g_ref[...])
        low = [v[half:, :] for v in gg]
        symmetric(w_ref, dot3([v[:half, :] for v in gg], gg, dims), dot3(low, low, dims))

    @pl.when(c == 1)
    def _():
        dims = (((0,), (0,)), ((), ()))
        gg = split(g_ref[...])
        low = [v[:, half:] for v in gg]
        symmetric(w_ref, dot3([v[:, :half] for v in gg], gg, dims), dot3(low, low, dims))

    stat = w_ref[...] + jnp.where(eye, ridge, 0.0)
    w_ref[...] = stat
    mag = jnp.sqrt(jnp.sum(stat * stat, keepdims=True))
    s_ref[...] = jnp.broadcast_to(SCALE0 * lax.rsqrt(jnp.sqrt(mag)), s_ref.shape)
    n_ref[...] = w_ref[...] * (0.2 / mag)


def chain(n_ref, d_ref, w_ref, v_ref, m_ref, r_ref, parts, dot):
    def advance(src, dst):
        n = parts(src[...])
        product_into(w_ref, n, n, dot)
        product_into(v_ref, n, parts(w_ref[...]), dot)
        v_ref[...] = src[...] - 2.0 * w_ref[...] + v_ref[...]
        product_into(dst, parts(w_ref[...] - 2.0 * src[...]), parts(v_ref[...]), dot)
        dst[...] = (1.25**4) * (v_ref[...] + dst[...])

    advance(n_ref, m_ref)
    product_into(r_ref, parts(n_ref[...]), parts(m_ref[...]), dot)
    r_ref[...] = n_ref[...] + m_ref[...] - r_ref[...]
    advance(m_ref, n_ref)
    product_into(d_ref, parts(r_ref[...]), parts(n_ref[...]), dot)
    d_ref[...] = r_ref[...] + n_ref[...] - d_ref[...]


PAIRS = [(i, j) for i in range(4) for j in range(i, 4)]
MID = 16
PIECE = len(PAIRS) * 128 // MID


def exchange(box, value, me, n, dev_of, s, r):
    box[me] = value
    for d in range(1, n):
        remote(box.at[me], box.at[me], s, r, dev_of((me + d) % n)).start()


def exchanged(box, me, n, dev_of, s, r):
    ref = box.at[0 : n - 1]
    remote(ref, ref, s, r, dev_of(me)).wait_recv()
    total = box[0]
    for i in range(1, n):
        total = total + box[i]
    return total


def sent(box, me, n, dev_of, s, r):
    ref = box.at[0 : n - 1]
    remote(ref, ref, s, r, dev_of(me)).wait_send()


def finish_stage(
    src, g, dev, scale, root_refs, pbox, root, graft,
    bbox, dhi, dlo, phi, plo, pscale, pack, abox, stage, t_ref, pout, box1, box2, box3,
    d_s, d_r, a_s, a_r, b_s, b_r, o_s, o_r, e1_s, e1_r, e2_s, e2_r, e3_s, e3_r,
):
    z, x, y, c = coords()
    kappa, xs = x // 2, x % 2
    other = (z, x, y, 1 - c)
    half = B // 2

    n_ref, w_ref, v_ref, m_ref, r_ref = root_refs
    for n, (i, j) in enumerate(PAIRS):
        pack[n * 128 : (n + 1) * 128, :] = n_ref[i * 128 : (i + 1) * 128, j * 128 : (j + 1) * 128].astype(bf16)
    sv = scale[0:1, 0:1]
    s0 = sv.astype(bf16).astype(f32)
    s1 = (sv - s0).astype(bf16).astype(f32)
    s2 = sv - s0 - s1
    row = lax.broadcasted_iota(jnp.int32, (16, 128), 0)
    col = lax.broadcasted_iota(jnp.int32, (16, 128), 1)
    end = pack.shape[0]
    last = pack[end - 16 : end, :].astype(f32)
    for k, v in enumerate((s0, s1, s2)):
        last = jnp.where((row == 15) & (col == k), v, last)
    pack[end - 16 : end, :] = last.astype(bf16)

    mine = z * 4 + 2 * c + xs
    forwards = xs == c
    k_me = z * 2 + x // 2

    def leg_a(k):
        rows = pl.ds(pl.multiple_of(k * PIECE, 16), PIECE)
        return remote(
            pack.at[rows], abox.at[mine], a_s, a_r, (k // 2, 2 * (k % 2) + kappa, y, kappa)
        )

    def is_me(k):
        return (k == k_me) & forwards & (kappa == c)

    far_first = (4, 3, 5, 2, 6, 1, 7, 0)
    for t in range(MID):
        k = (2 * (z + far_first[t // 2]) + t % 2) % MID

        @pl.when(jnp.logical_not(is_me(k)))
        def _():
            leg_a(k).start()

    @pl.when(forwards & (kappa == c))
    def _():
        abox[mine] = pack[pl.ds(pl.multiple_of(k_me * PIECE, 16), PIECE), :]

    chain(n_ref, dev, w_ref, v_ref, m_ref, r_ref, split, dot3)
    dhi[...] = dev[...].astype(bf16)
    dlo[...] = (dev[...] - dhi[...].astype(f32)).astype(bf16)

    def cross(lo):
        rows = pl.ds(lo, B - lo)
        return [
            remote(dhi.at[rows], phi.at[rows], d_s.at[0], d_r.at[0], other),
            remote(dlo.at[rows], plo.at[rows], d_s.at[1], d_r.at[1], other),
            remote(scale, pscale, d_s.at[2], d_r.at[2], other),
        ]

    @pl.when(c == 0)
    def _():
        for t in cross(half):
            t.start()

    @pl.when(c == 1)
    def _():
        for t in cross(0):
            t.start()

    @pl.when(c == 0)
    def _():
        t_ref[:half, :] = g[:half, :] - dot3((dhi[:half, :], dlo[:half, :]), split(g[...]))

    @pl.when(c == 1)
    def _():
        t_ref[...] = g[...] - dot3(split(g[...]), (dhi[...], dlo[...]))

    @pl.when(c == 0)
    def _():
        high, low, scales = cross(0)
        u = t_ref[:half, :]
        uh, ul = split(u)
        high.wait_recv()
        first = jnp.dot(uh, phi[...], preferred_element_type=f32) + jnp.dot(ul, phi[...], preferred_element_type=f32)
        low.wait_recv()
        scales.wait_recv()
        factor = scale[0:1, 0:1] * pscale[0:1, 0:1]
        p = factor * (u - (first + jnp.dot(uh, plo[...], preferred_element_type=f32)))
        pout[0] = p[:128, :]
        pout[1] = p[128:, :]

    @pl.when(c == 1)
    def _():
        for t in cross(half):
            t.wait_recv()
        factor = scale[0:1, 0:1] * pscale[0:1, 0:1]
        tt = split(t_ref[...])
        for r in range(2):
            rows = slice(half + r * 128, half + (r + 1) * 128)
            pout[r] = factor * (t_ref[rows, :] - dot3((phi[rows, :], plo[rows, :]), tt))

    sum_p = jnp.sum(pout[...] * pout[...], axis=0)
    sum_p = jnp.sum(sum_p, keepdims=True)
    sum_g = 0.5 * jnp.sum(g[...] * g[...], keepdims=True)
    row8 = lax.broadcasted_iota(jnp.int32, (8, 128), 0)
    value = jnp.where(row8 == 0, sum_p, jnp.where(row8 == 1, sum_g, 0.0))

    e1 = (box1, x * 2 + c, 2 * NX, lambda i: (z, i // 2, y, i % 2), e1_s, e1_r)
    e2 = (box2, y, NY, lambda i: (z, x, i, c), e2_s, e2_r)
    e3 = (box3, z, NZ, lambda i: (i, x, y, c), e3_s, e3_r)
    exchange(e1[0], value, *e1[1:])


    def rows_to(r):
        return remote(
            pout.at[r], pbox.at[:, pl.ds(pl.multiple_of(xs * B, B), B)], o_s.at[r], o_r.at[xs], (z, 2 * c + r, y, kappa)
        )

    def place_b(t):
        return (z + far_first[t // NX]) % NZ, (x + NX - 1 - t % NX) % NX

    def leg_b(t):
        zd, xd = place_b(t)
        return remote(stage.at[t], bbox.at[k_me], b_s, b_r, (zd, xd, y, c))

    @pl.when(forwards)
    def _():
        for there in range(2):
            @pl.when((kappa == c) == bool(there))
            def _():
                ref = abox.at[0 : NZ * NX - there]
                remote(ref, ref, a_s, a_r, other).wait_recv()
        for t in range(NZ * NX):
            zd, xd = place_b(t)
            piece = abox[src[zd * NX + xd]]
            if t < NZ * NX - 1:
                stage[t] = piece
            else:
                bbox[k_me] = piece
        for t in range(NZ * NX - 1):
            leg_b(t).start()
    for r in range(2):
        @pl.when(2 * c + r != x)
        def _():
            rows_to(r).start()

        @pl.when(2 * c + r == x)
        def _():
            pbox[:, pl.ds(pl.multiple_of(xs * B, B), B)] = pout[r]

    exchange(e2[0], exchanged(*e1), *e2[1:])
    exchange(e3[0], exchanged(*e2), *e3[1:])

    for there in range(2):
        @pl.when(forwards == bool(there))
        def _():
            ref = bbox.at[0 : MID - there]
            remote(ref, ref, b_s, b_r, other).wait_recv()

    row = lax.broadcasted_iota(jnp.int32, (128, 128), 0)
    col = lax.broadcasted_iota(jnp.int32, (128, 128), 1)
    whole = bbox[...].reshape(MID * PIECE, 128)
    for n, (i, j) in enumerate(PAIRS):
        block = whole[n * 128 : (n + 1) * 128, :].astype(f32)
        if i != j:
            n_ref[j * 128 : (j + 1) * 128, i * 128 : (i + 1) * 128] = block.T
        elif i == 3:
            corner = block[127:128, :]
            got = corner[:, 0:1] + corner[:, 1:2] + corner[:, 2:3]
            block = jnp.where((row == 127) & (col < 3), block.T, block)
        n_ref[i * 128 : (i + 1) * 128, j * 128 : (j + 1) * 128] = block
    chain(n_ref, dev, w_ref, v_ref, m_ref, r_ref, lambda v: (v.astype(bf16),), dot1)
    eye = lax.broadcasted_iota(jnp.int32, (B, B), 0) == lax.broadcasted_iota(jnp.int32, (B, B), 1)
    root[...] = got * (jnp.where(eye, 1.0, 0.0) - dev[...])
    total = exchanged(*e3)
    graft[...] = jnp.broadcast_to(jnp.sqrt(total[1:2, :] / jnp.maximum(total[0:1, :], 1.0)), graft.shape)

    for s in range(2):
        @pl.when(2 * c + s != x)
        def _():
            ref = pbox.at[:, s * B : (s + 1) * B]
            remote(ref, ref, o_s.at[0], o_r.at[s], other).wait_recv()

    @pl.when(c == 0)
    def _():
        for t in cross(half):
            t.wait_send()

    @pl.when(c == 1)
    def _():
        for t in cross(0):
            t.wait_send()

    for there in range(2):
        @pl.when((forwards & (kappa == c)) == bool(there))
        def _():
            ref = pack.at[0 : (MID - there) * PIECE]
            remote(ref, ref, a_s, a_r, other).wait_send()

    for r in range(2):
        @pl.when(2 * c + r != x)
        def _():
            rows_to(r).wait_send()

    @pl.when(forwards)
    def _():
        ref = stage.at[0 : NZ * NX - 1]
        remote(ref, ref, b_s, b_r, other).wait_send()

    for e in (e1, e2, e3):
        sent(*e)


N_GRAD = 6 + 15
N_ROOT = 5


def step_kernel(owners, act, cot, pbox, root, graft, g, dev, scale, own, src, own_sem, *refs):
    grad, spare, rest = refs[:N_GRAD], refs[N_GRAD : N_GRAD + N_ROOT], refs[N_GRAD + N_ROOT :]
    load = pltpu.make_async_copy(owners, own, own_sem)
    load.start()

    def table():
        load.wait()

        def entry(d, carry):
            place = jnp.int32(0)
            for b in range(NB):
                at = (b // 2) * 4 + b % 2
                o = own[b]
                place = jnp.where(o == d, at, place)
                place = jnp.where(o + 1 - 2 * (o % 2) == d, at + 2, place)
            src[d] = place
            return carry

        lax.fori_loop(0, NZ * NX, entry, 0)

    gradient_stage(act, cot, g, table, *grad)
    statistic_stage(g, scale, spare[0], spare[1])
    finish_stage(src, g, dev, scale, spare, pbox, root, graft, *rest)


def step(owners, act, cot):
    dma = pltpu.SemaphoreType.DMA
    vmem = pltpu.VMEM
    in_vmem = pl.BlockSpec(memory_space=pltpu.VMEM)
    return pl.pallas_call(
        step_kernel,
        out_shape=(
            jax.ShapeDtypeStruct((B // NX, CB * B), f32),
            jax.ShapeDtypeStruct((B, B), f32),
            jax.ShapeDtypeStruct((8, 128), f32),
        ),
        in_specs=[pl.BlockSpec(memory_space=pltpu.HBM)] * 3,
        out_specs=(in_vmem,) * 3,
        scratch_shapes=[
            vmem((B, B), f32), vmem((B, B), f32), vmem((8, 128), f32),
            pltpu.SMEM((NB,), jnp.int32), pltpu.SMEM((NZ * NX,), jnp.int32), pltpu.SemaphoreType.DMA,
            vmem((NZ, 2, NY, TY, B), bf16),
            vmem((NZ, 2, T, B), bf16),
            vmem((TY, NZ * B), bf16),
            vmem((T, CB * B), bf16),
            vmem((4, B // 4, B), f32),
            vmem((4, B // 4, B), f32),
            dma((2,)),
            dma((2,)), dma((2,)),
            dma, dma((NZ,)),
            dma, dma((NY * 4,)),
            dma, dma((16,)),
            dma, dma((16,)),
            dma((2,)), dma((NY * 4,)),
            dma((4,)), dma((4,)),
            *[vmem((B, B), f32)] * N_ROOT,
            vmem((MID, PIECE, 128), bf16),
            vmem((B, B), bf16), vmem((B, B), bf16), vmem((B, B), bf16), vmem((B, B), bf16),
            vmem((8, 128), f32),
            vmem((MID * PIECE, 128), bf16),
            vmem((NZ * NX, PIECE, 128), bf16),
            vmem((NZ * NX, PIECE, 128), bf16),
            vmem((B, B), f32),
            vmem((2, 128, B), f32),
            vmem((8, 8, 128), f32), vmem((8, 8, 128), f32), vmem((8, 8, 128), f32),
            dma((3,)), dma((3,)),
            dma, dma, dma, dma,
            dma((2,)), dma((2,)),
            dma, dma, dma, dma, dma, dma,
        ],
        compiler_params=pltpu.CompilerParams(
            collective_id=0, has_side_effects=True, vmem_limit_bytes=52 * 2**20
        ),
        name="step",
    )(owners, act, cot)


def output_kernel(pbox, root_in, graft, update, root, factor, sem):
    copy = pltpu.make_async_copy(root_in, root, sem)
    copy.start()
    update[...] = (graft[0:1, 0:1] * pbox[...]).astype(bf16)
    factor[...] = graft[0:1, 0:1]
    copy.wait()


def outputs(pbox, root, graft):
    vmem = pl.BlockSpec(memory_space=pltpu.VMEM)
    anyw = pl.BlockSpec(memory_space=pl.ANY)
    return pl.pallas_call(
        output_kernel,
        out_shape=(
            jax.ShapeDtypeStruct((B // NX, CB * B), bf16),
            jax.ShapeDtypeStruct((B, B), f32),
            jax.ShapeDtypeStruct((1, 1), f32),
        ),
        in_specs=[vmem, anyw, vmem],
        out_specs=(vmem, anyw, vmem),
        scratch_shapes=[pltpu.SemaphoreType.DMA],
        compiler_params=pltpu.CompilerParams(vmem_limit_bytes=8 * 2**20),
        name="outputs",
    )(pbox, root, graft)


def on_device(act, cot, owners):
    update, root, graft = outputs(*step(owners, act, cot))
    return update, root, graft.reshape(())


def solution(mesh):
    finer = Mesh(mesh.devices.reshape(NZ, NX, NY, 2), ("z", "x", "y", "c"))
    dp, mp = ("z", "x"), ("y", "c")
    return jax.shard_map(
        on_device,
        mesh=finer,
        in_specs=(P(dp, None), P(dp, mp), P()),
        out_specs=(P(dp, mp), P(dp, mp), P()),
        check_vma=False,
    )
```

```python
import functools

import jax
import jax.numpy as jnp
from jax import lax
from jax.experimental import pallas as pl
from jax.experimental.pallas import tpu as pltpu
from jax.sharding import Mesh
from jax.sharding import PartitionSpec as P

B = 512
CB = 2
NZ, NX, NY = 8, 4, 8
NB = 16
T = 128
TY = T // NY
MESH_ID = pl.DeviceIdType.MESH
f32, bf16 = jnp.float32, jnp.bfloat16


def remote(src, dst, s, r, dev):
    return pltpu.make_async_remote_copy(
        src_ref=src, dst_ref=dst, send_sem=s, recv_sem=r, device_id=dev, device_id_type=MESH_ID
    )


def coords():
    return tuple(lax.axis_index(n) for n in ("z", "x", "y", "c"))


def gradient_stage(
    act, cot, g_out, table, abuf, cbuf, amine, cmine, psend, precv,
    ld_sem, c1_s, c1_r, a1_s, a1_r, a2_s, a2_r, cr_s, cr_r, ar_s, ar_r, w_s, w_r, p_s, p_r,
):
    z, x, y, c = coords()
    active = x // 2 == c
    xs = x % 2

    load_c = pltpu.make_async_copy(cot, cmine, ld_sem.at[0])
    load_a = pltpu.make_async_copy(act.at[pl.ds(pl.multiple_of(y * TY, TY), TY), :], amine, ld_sem.at[1])
    load_c.start()
    load_a.start()

    @pl.when(active)
    def _():
        for h in range(2):
            @pl.when(xs == h)
            def _():
                pltpu.make_async_copy(
                    cot.at[:, h * B : (h + 1) * B], cbuf.at[z, xs], c1_r.at[xs]
                ).start()
        pltpu.make_async_copy(
            act.at[pl.ds(pl.multiple_of(y * TY, TY), TY), pl.ds(pl.multiple_of(z * B, B), B)],
            abuf.at[z, xs, y],
            a1_r.at[0],
        ).start()

    bar = pltpu.get_barrier_semaphore()

    def hello(*dev):
        pl.semaphore_signal(bar, inc=1, device_id=dev, device_id_type=MESH_ID)

    for d in range(1, 2 * NX * NZ):
        g = (z * 2 * NX + x * 2 + c + d) % (2 * NX * NZ)
        hello(g // (2 * NX), g // 2 % NX, y, g % 2)
    for d in range(1, NY):
        hello(z, x, (y + d) % NY, c)
    pl.semaphore_wait(bar, 2 * NX * NZ - 1 + NY - 1)

    load_c.wait()
    load_a.wait()

    def c1(h):
        return remote(
            cmine.at[:, h * B : (h + 1) * B], cbuf.at[z, xs], c1_s.at[h], c1_r.at[xs], (z, 2 * c + h, y, x // 2)
        )

    for h in range(2):
        @pl.when(2 * c + h != x)
        def _():
            c1(h).start()

    def a1(d):
        zd = (z + d) % NZ
        return remote(
            amine.at[:, pl.ds(pl.multiple_of(zd * B, B), B)], abuf.at[z, xs, y], a1_s, a1_r.at[d], (zd, x, y, c)
        )

    @pl.when(active)
    def _():
        for d in (4, 3, 5, 2, 6, 1, 7):
            a1(d).start()

    table()

    half = NZ // 2
    c_moves = [(s, o, d) for s in range(1, half) for o in range(2) for d in (1, -1)] + [(half, 0, 1), (half, 1, -1)]

    def c_move(step, o, direction, back):
        chunk = (z + NZ - direction * (step - 1 + back)) % NZ
        ref = cbuf.at[chunk, o]
        i = (step - 1) * 4 + o * 2 + (direction > 0)
        return remote(ref, ref, cr_s, cr_r.at[i], ((z + NZ + direction) % NZ, x, y, c))

    def c_step(step):
        for o in range(2):
            for d in (1, -1):
                if (step, o, d) in c_moves:
                    c_move(step, o, d, 1).wait_recv()
                if (step + 1, o, d) in c_moves:
                    c_move(step + 1, o, d, 0).start()

    offsets = (0, -1, 1, -2, 2, -3, 3, 4)
    halves = (slice(0, half), slice(half, NZ))

    def at_y(q):
        return (y + NY + offsets[q]) % NY

    def y_move(step, direction, back, part):
        k = (y + NY - direction * (step - 1 + back)) % NY
        ref = abuf.at[halves[part], xs, k]
        i = (step - 1) * 4 + part * 2 + (direction > 0)
        return remote(ref, ref, ar_s, ar_r.at[i], (z, x, (y + NY + direction) % NY, c))

    def y_parts(step, direction):
        return (0, 1) if step < NY // 2 else (int(direction < 0),)

    def x_move(q, s, direction):
        ref = abuf.at[:, s, at_y(q)]
        i = q * 4 + s * 2 + (direction > 0)
        return remote(ref, ref, a2_s, a2_r.at[i], (z, (x + NX + direction) % NX, y, c))

    def x_half(q, s, direction):
        ref = abuf.at[halves[direction < 0], s, at_y(q)]
        i = q * 4 + s * 2 + (direction > 0)
        return remote(ref, ref, w_s.at[s], w_r.at[i], (z, (x + NX + direction) % NX, y, c))

    def x_start(q):
        for d in (1, -1):
            x_move(q, xs, d).start()

    def x_relay(q):
        for s in range(2):
            for d, place in ((1, 1), (-1, 3)):
                @pl.when((x + NX - 2 * c - s) % NX == place)
                def _():
                    x_move(q, s, d).wait_recv()
                    x_half(q, s, d).start()

    def y_step(step):
        @pl.when(active)
        def _():
            for part in range(2):
                for d in (1, -1):
                    if part in y_parts(step, d):
                        y_move(step, d, 1, part).wait_recv()
                    if step < NY // 2 and part in y_parts(step + 1, d):
                        y_move(step + 1, d, 0, part).start()
            if step < NY // 2:
                x_start(2 * step - 1)
                x_start(2 * step)
            else:
                x_start(NY - 1)

    for o in range(2):
        c1_wait = remote(cbuf.at[z, o], cbuf.at[z, o], c1_s.at[0], c1_r.at[o], (z, x, y, c))
        c1_wait.wait_recv()
        for d in (1, -1):
            c_move(1, o, d, 0).start()

    @pl.when(active)
    def _():
        for d in range(NZ):
            ref = abuf.at[(z + NZ - d) % NZ, xs, y]
            remote(ref, ref, a1_s, a1_r.at[d], (z, x, y, c)).wait_recv()
        for part in range(2):
            for d in (1, -1):
                y_move(1, d, 0, part).start()
        x_start(0)

    y_step(1)
    x_relay(0)
    c_step(1)
    y_step(2)
    x_relay(1)
    y_step(3)
    c_step(2)
    y_step(4)
    x_relay(2)
    x_relay(3)
    x_relay(4)
    c_step(3)
    x_relay(5)
    x_relay(6)
    x_relay(7)
    c_step(4)
    for s in range(2):
        @pl.when((x + NX - 2 * c - s) % NX == 2)
        def _():
            for q in range(NY):
                for d in (1, -1):
                    x_half(q, s, d).wait_recv()

    def pcopy(r):
        return remote(psend.at[r], precv.at[r], p_s.at[r], p_r.at[r], (z, x, y, 1 - c))

    rows = B // 4
    cot_all = cbuf[...].reshape(NZ * 2 * T, B)
    for r in range(4):
        lhs = abuf[:, :, :, :, r * rows : (r + 1) * rows].reshape(NZ * 2 * T, rows)
        part = lax.dot_general(lhs, cot_all, (((0,), (0,)), ((), ())), preferred_element_type=f32)
        psend[r] = part * (1.0 / 64.0)
        pcopy(r).start()

    for h in range(2):
        @pl.when(2 * c + h != x)
        def _():
            c1(h).wait_send()

    @pl.when(active)
    def _():
        remote(abuf.at[0:7, 0, y], abuf.at[0:7, 0, y], a1_s, a1_r.at[0], (z, x, y, c)).wait_send()
        line = abuf.at[0:7, 0]
        remote(line, line, ar_s, ar_r.at[0], (z, x, y, c)).wait_send()
        line = abuf.at[:, :, :]
        remote(line, line, a2_s, a2_r.at[0], (z, x, y, c)).wait_send()

    for s in range(2):
        @pl.when((x + NX - 2 * c - s) % 2 == 1)
        def _():
            line = abuf.at[0:half, 0]
            remote(line, line, w_s.at[s], w_r.at[0], (z, x, y, c)).wait_send()

    line = cbuf.at[0:7]
    remote(line, line, cr_s, cr_r.at[0], (z, x, y, c)).wait_send()
    for r in range(4):
        pcopy(r).wait_recv()
        g_out[r * rows : (r + 1) * rows, :] = psend[r] + precv[r]
    for r in range(4):
        pcopy(r).wait_send()


def split(v):
    hi = v.astype(bf16)
    return hi, (v - hi.astype(f32)).astype(bf16)


def dot3(a, b, dims=(((1,), (0,)), ((), ()))):
    def d(p, q):
        return lax.dot_general(p, q, dims, preferred_element_type=f32)

    return d(a[0], b[0]) + (d(a[0], b[1]) + d(a[1], b[0]))


def dot1(a, b):
    return jnp.dot(a[0], b[0], preferred_element_type=f32)


def symmetric(ref, top, low):
    half = B // 2
    ref[:half, :] = top
    ref[half:, :half] = top[:, half:].T
    ref[half:, half:] = low


def product_into(ref, a, b, dot):
    half = B // 2
    top = dot([v[:half, :] for v in a], b)
    symmetric(ref, top, dot([v[half:, :] for v in a], [v[:, half:] for v in b]))


SCALE0 = 1.25**3


def statistic_stage(g_ref, s_ref, n_ref, w_ref):
    c = lax.axis_index("c")
    g = g_ref[...]
    ridge = 0.1 * (jnp.sum(g * g, keepdims=True) / B + 1.0)
    eye = lax.broadcasted_iota(jnp.int32, (B, B), 0) == lax.broadcasted_iota(jnp.int32, (B, B), 1)

    half = B // 2

    @pl.when(c == 0)
    def _():
        dims = (((1,), (1,)), ((), ()))
        gg = split(g_ref[...])
        low = [v[half:, :] for v in gg]
        symmetric(w_ref, dot3([v[:half, :] for v in gg], gg, dims), dot3(low, low, dims))

    @pl.when(c == 1)
    def _():
        dims = (((0,), (0,)), ((), ()))
        gg = split(g_ref[...])
        low = [v[:, half:] for v in gg]
        symmetric(w_ref, dot3([v[:, :half] for v in gg], gg, dims), dot3(low, low, dims))

    stat = w_ref[...] + jnp.where(eye, ridge, 0.0)
    w_ref[...] = stat
    mag = jnp.sqrt(jnp.sum(stat * stat, keepdims=True))
    s_ref[...] = jnp.broadcast_to(SCALE0 * lax.rsqrt(jnp.sqrt(mag)), s_ref.shape)
    n_ref[...] = w_ref[...] * (0.2 / mag)


def chain(n_ref, d_ref, w_ref, v_ref, m_ref, r_ref, parts, dot):
    def advance(src, dst):
        n = parts(src[...])
        product_into(w_ref, n, n, dot)
        product_into(v_ref, n, parts(w_ref[...]), dot)
        v_ref[...] = src[...] - 2.0 * w_ref[...] + v_ref[...]
        product_into(dst, parts(w_ref[...] - 2.0 * src[...]), parts(v_ref[...]), dot)
        dst[...] = (1.25**4) * (v_ref[...] + dst[...])

    advance(n_ref, m_ref)
    product_into(r_ref, parts(n_ref[...]), parts(m_ref[...]), dot)
    r_ref[...] = n_ref[...] + m_ref[...] - r_ref[...]
    advance(m_ref, n_ref)
    product_into(d_ref, parts(r_ref[...]), parts(n_ref[...]), dot)
    d_ref[...] = r_ref[...] + n_ref[...] - d_ref[...]


PAIRS = [(i, j) for i in range(4) for j in range(i, 4)]
MID = 16
PIECE = len(PAIRS) * 128 // MID


def exchange(box, value, me, n, dev_of, s, r):
    box[me] = value
    for d in range(1, n):
        remote(box.at[me], box.at[me], s, r, dev_of((me + d) % n)).start()


def exchanged(box, me, n, dev_of, s, r):
    ref = box.at[0 : n - 1]
    remote(ref, ref, s, r, dev_of(me)).wait_recv()
    total = box[0]
    for i in range(1, n):
        total = total + box[i]
    return total


def sent(box, me, n, dev_of, s, r):
    ref = box.at[0 : n - 1]
    remote(ref, ref, s, r, dev_of(me)).wait_send()


def finish_stage(
    src, g, dev, scale, root_refs, pbox, root, graft,
    bbox, dhi, dlo, phi, plo, pscale, pack, abox, stage, t_ref, pout, box1, box2, box3,
    d_s, d_r, a_s, a_r, b_s, b_r, o_s, o_r, e1_s, e1_r, e2_s, e2_r, e3_s, e3_r,
):
    z, x, y, c = coords()
    kappa, xs = x // 2, x % 2
    other = (z, x, y, 1 - c)
    half = B // 2

    n_ref, w_ref, v_ref, m_ref, r_ref = root_refs
    for n, (i, j) in enumerate(PAIRS):
        pack[n * 128 : (n + 1) * 128, :] = n_ref[i * 128 : (i + 1) * 128, j * 128 : (j + 1) * 128].astype(bf16)
    sv = scale[0:1, 0:1]
    s0 = sv.astype(bf16).astype(f32)
    s1 = (sv - s0).astype(bf16).astype(f32)
    s2 = sv - s0 - s1
    row = lax.broadcasted_iota(jnp.int32, (16, 128), 0)
    col = lax.broadcasted_iota(jnp.int32, (16, 128), 1)
    end = pack.shape[0]
    last = pack[end - 16 : end, :].astype(f32)
    for k, v in enumerate((s0, s1, s2)):
        last = jnp.where((row == 15) & (col == k), v, last)
    pack[end - 16 : end, :] = last.astype(bf16)

    mine = z * 4 + 2 * c + xs
    forwards = xs == c
    k_me = z * 2 + x // 2

    def leg_a(k):
        rows = pl.ds(pl.multiple_of(k * PIECE, 16), PIECE)
        return remote(
            pack.at[rows], abox.at[mine], a_s, a_r, (k // 2, 2 * (k % 2) + kappa, y, kappa)
        )

    def is_me(k):
        return (k == k_me) & forwards & (kappa == c)

    far_first = (4, 3, 5, 2, 6, 1, 7, 0)
    for t in range(MID):
        k = (2 * (z + far_first[t // 2]) + t % 2) % MID

        @pl.when(jnp.logical_not(is_me(k)))
        def _():
            leg_a(k).start()

    @pl.when(forwards & (kappa == c))
    def _():
        abox[mine] = pack[pl.ds(pl.multiple_of(k_me * PIECE, 16), PIECE), :]

    chain(n_ref, dev, w_ref, v_ref, m_ref, r_ref, split, dot3)
    dhi[...] = dev[...].astype(bf16)
    dlo[...] = (dev[...] - dhi[...].astype(f32)).astype(bf16)

    def cross(lo):
        rows = pl.ds(lo, B - lo)
        return [
            remote(dhi.at[rows], phi.at[rows], d_s.at[0], d_r.at[0], other),
            remote(dlo.at[rows], plo.at[rows], d_s.at[1], d_r.at[1], other),
            remote(scale, pscale, d_s.at[2], d_r.at[2], other),
        ]

    @pl.when(c == 0)
    def _():
        for t in cross(half):
            t.start()

    @pl.when(c == 1)
    def _():
        for t in cross(0):
            t.start()

    @pl.when(c == 0)
    def _():
        t_ref[:half, :] = g[:half, :] - dot3((dhi[:half, :], dlo[:half, :]), split(g[...]))

    @pl.when(c == 1)
    def _():
        t_ref[...] = g[...] - dot3(split(g[...]), (dhi[...], dlo[...]))

    sum_g = 0.5 * jnp.sum(g[...] * g[...], keepdims=True)
    @pl.when(c == 0)
    def _():
        high, low, scales = cross(0)
        u = t_ref[:half, :]
        uh, ul = split(u)
        high.wait_recv()
        first = jnp.dot(uh, phi[...], preferred_element_type=f32) + jnp.dot(ul, phi[...], preferred_element_type=f32)
        low.wait_recv()
        scales.wait_recv()
        factor = scale[0:1, 0:1] * pscale[0:1, 0:1]
        p = factor * (u - (first + jnp.dot(uh, plo[...], preferred_element_type=f32)))
        pout[0] = p[:128, :]
        pout[1] = p[128:, :]

    @pl.when(c == 1)
    def _():
        for t in cross(half):
            t.wait_recv()
        factor = scale[0:1, 0:1] * pscale[0:1, 0:1]
        tt = split(t_ref[...])
        for r in range(2):
            rows = slice(half + r * 128, half + (r + 1) * 128)
            pout[r] = factor * (t_ref[rows, :] - dot3((phi[rows, :], plo[rows, :]), tt))

    sum_p = jnp.sum(pout[...] * pout[...], axis=0)
    sum_p = jnp.sum(sum_p, keepdims=True)
    row8 = lax.broadcasted_iota(jnp.int32, (8, 128), 0)
    value = jnp.where(row8 == 0, sum_p, jnp.where(row8 == 1, sum_g, 0.0))

    e1 = (box1, x * 2 + c, 2 * NX, lambda i: (z, i // 2, y, i % 2), e1_s, e1_r)
    e2 = (box2, y, NY, lambda i: (z, x, i, c), e2_s, e2_r)
    e3 = (box3, z, NZ, lambda i: (i, x, y, c), e3_s, e3_r)
    exchange(e1[0], value, *e1[1:])


    def rows_to(r):
        return remote(
            pout.at[r], pbox.at[:, pl.ds(pl.multiple_of(xs * B, B), B)], o_s.at[r], o_r.at[xs], (z, 2 * c + r, y, kappa)
        )

    def place_b(t):
        return (z + far_first[t // NX]) % NZ, (x + NX - 1 - t % NX) % NX

    def leg_b(t):
        zd, xd = place_b(t)
        return remote(stage.at[t], bbox.at[k_me], b_s, b_r, (zd, xd, y, c))

    @pl.when(forwards)
    def _():
        for there in range(2):
            @pl.when((kappa == c) == bool(there))
            def _():
                ref = abox.at[0 : NZ * NX - there]
                remote(ref, ref, a_s, a_r, other).wait_recv()
        for t in range(NZ * NX):
            zd, xd = place_b(t)
            piece = abox[src[zd * NX + xd]]
            if t < NZ * NX - 1:
                stage[t] = piece
            else:
                bbox[k_me] = piece
        for t in range(NZ * NX - 1):
            leg_b(t).start()
    for r in range(2):
        @pl.when(2 * c + r != x)
        def _():
            rows_to(r).start()

        @pl.when(2 * c + r == x)
        def _():
            pbox[:, pl.ds(pl.multiple_of(xs * B, B), B)] = pout[r]

    exchange(e2[0], exchanged(*e1), *e2[1:])
    exchange(e3[0], exchanged(*e2), *e3[1:])

    for there in range(2):
        @pl.when(forwards == bool(there))
        def _():
            ref = bbox.at[0 : MID - there]
            remote(ref, ref, b_s, b_r, other).wait_recv()

    row = lax.broadcasted_iota(jnp.int32, (128, 128), 0)
    col = lax.broadcasted_iota(jnp.int32, (128, 128), 1)
    whole = bbox[...].reshape(MID * PIECE, 128)
    for n, (i, j) in enumerate(PAIRS):
        block = whole[n * 128 : (n + 1) * 128, :].astype(f32)
        if i != j:
            n_ref[j * 128 : (j + 1) * 128, i * 128 : (i + 1) * 128] = block.T
        elif i == 3:
            corner = block[127:128, :]
            got = corner[:, 0:1] + corner[:, 1:2] + corner[:, 2:3]
            block = jnp.where((row == 127) & (col < 3), block.T, block)
        n_ref[i * 128 : (i + 1) * 128, j * 128 : (j + 1) * 128] = block
    chain(n_ref, dev, w_ref, v_ref, m_ref, r_ref, lambda v: (v.astype(bf16),), dot1)
    eye = lax.broadcasted_iota(jnp.int32, (B, B), 0) == lax.broadcasted_iota(jnp.int32, (B, B), 1)
    root[...] = got * (jnp.where(eye, 1.0, 0.0) - dev[...])
    total = exchanged(*e3)
    graft[...] = jnp.broadcast_to(jnp.sqrt(total[1:2, :] / jnp.maximum(total[0:1, :], 1.0)), graft.shape)

    for s in range(2):
        @pl.when(2 * c + s != x)
        def _():
            ref = pbox.at[:, s * B : (s + 1) * B]
            remote(ref, ref, o_s.at[0], o_r.at[s], other).wait_recv()

    @pl.when(c == 0)
    def _():
        for t in cross(half):
            t.wait_send()

    @pl.when(c == 1)
    def _():
        for t in cross(0):
            t.wait_send()

    for there in range(2):
        @pl.when((forwards & (kappa == c)) == bool(there))
        def _():
            ref = pack.at[0 : (MID - there) * PIECE]
            remote(ref, ref, a_s, a_r, other).wait_send()

    for r in range(2):
        @pl.when(2 * c + r != x)
        def _():
            rows_to(r).wait_send()

    @pl.when(forwards)
    def _():
        ref = stage.at[0 : NZ * NX - 1]
        remote(ref, ref, b_s, b_r, other).wait_send()

    for e in (e1, e2, e3):
        sent(*e)


N_GRAD = 6 + 15
N_ROOT = 5


def step_kernel(owners, act, cot, pbox, root, graft, g, dev, scale, own, src, own_sem, *refs):
    grad, spare, rest = refs[:N_GRAD], refs[N_GRAD : N_GRAD + N_ROOT], refs[N_GRAD + N_ROOT :]
    load = pltpu.make_async_copy(owners, own, own_sem)
    load.start()

    def table():
        load.wait()

        def entry(d, carry):
            place = jnp.int32(0)
            for b in range(NB):
                at = (b // 2) * 4 + b % 2
                o = own[b]
                place = jnp.where(o == d, at, place)
                place = jnp.where(o + 1 - 2 * (o % 2) == d, at + 2, place)
            src[d] = place
            return carry

        lax.fori_loop(0, NZ * NX, entry, 0)

    gradient_stage(act, cot, g, table, *grad)
    statistic_stage(g, scale, spare[0], spare[1])
    finish_stage(src, g, dev, scale, spare, pbox, root, graft, *rest)


def step(owners, act, cot):
    dma = pltpu.SemaphoreType.DMA
    vmem = pltpu.VMEM
    in_vmem = pl.BlockSpec(memory_space=pltpu.VMEM)
    return pl.pallas_call(
        step_kernel,
        out_shape=(
            jax.ShapeDtypeStruct((B // NX, CB * B), f32),
            jax.ShapeDtypeStruct((B, B), f32),
            jax.ShapeDtypeStruct((8, 128), f32),
        ),
        in_specs=[pl.BlockSpec(memory_space=pltpu.HBM)] * 3,
        out_specs=(in_vmem,) * 3,
        scratch_shapes=[
            vmem((B, B), f32), vmem((B, B), f32), vmem((8, 128), f32),
            pltpu.SMEM((NB,), jnp.int32), pltpu.SMEM((NZ * NX,), jnp.int32), pltpu.SemaphoreType.DMA,
            vmem((NZ, 2, NY, TY, B), bf16),
            vmem((NZ, 2, T, B), bf16),
            vmem((TY, NZ * B), bf16),
            vmem((T, CB * B), bf16),
            vmem((4, B // 4, B), f32),
            vmem((4, B // 4, B), f32),
            dma((2,)),
            dma((2,)), dma((2,)),
            dma, dma((NZ,)),
            dma, dma((NY * 4,)),
            dma, dma((16,)),
            dma, dma((16,)),
            dma((2,)), dma((NY * 4,)),
            dma((4,)), dma((4,)),
            *[vmem((B, B), f32)] * N_ROOT,
            vmem((MID, PIECE, 128), bf16),
            vmem((B, B), bf16), vmem((B, B), bf16), vmem((B, B), bf16), vmem((B, B), bf16),
            vmem((8, 128), f32),
            vmem((MID * PIECE, 128), bf16),
            vmem((NZ * NX, PIECE, 128), bf16),
            vmem((NZ * NX, PIECE, 128), bf16),
            vmem((B, B), f32),
            vmem((2, 128, B), f32),
            vmem((8, 8, 128), f32), vmem((8, 8, 128), f32), vmem((8, 8, 128), f32),
            dma((3,)), dma((3,)),
            dma, dma, dma, dma,
            dma((2,)), dma((2,)),
            dma, dma, dma, dma, dma, dma,
        ],
        compiler_params=pltpu.CompilerParams(
            collective_id=0, has_side_effects=True, vmem_limit_bytes=52 * 2**20
        ),
        name="step",
    )(owners, act, cot)


def output_kernel(pbox, root_in, graft, update, root, factor, sem):
    copy = pltpu.make_async_copy(root_in, root, sem)
    copy.start()
    update[...] = (graft[0:1, 0:1] * pbox[...]).astype(bf16)
    factor[...] = graft[0:1, 0:1]
    copy.wait()


def outputs(pbox, root, graft):
    vmem = pl.BlockSpec(memory_space=pltpu.VMEM)
    anyw = pl.BlockSpec(memory_space=pl.ANY)
    return pl.pallas_call(
        output_kernel,
        out_shape=(
            jax.ShapeDtypeStruct((B // NX, CB * B), bf16),
            jax.ShapeDtypeStruct((B, B), f32),
            jax.ShapeDtypeStruct((1, 1), f32),
        ),
        in_specs=[vmem, anyw, vmem],
        out_specs=(vmem, anyw, vmem),
        scratch_shapes=[pltpu.SemaphoreType.DMA],
        compiler_params=pltpu.CompilerParams(vmem_limit_bytes=8 * 2**20),
        name="outputs",
    )(pbox, root, graft)


def on_device(act, cot, owners):
    update, root, graft = outputs(*step(owners, act, cot))
    return update, root, graft.reshape(())


def solution(mesh):
    finer = Mesh(mesh.devices.reshape(NZ, NX, NY, 2), ("z", "x", "y", "c"))
    dp, mp = ("z", "x"), ("y", "c")
    return jax.shard_map(
        on_device,
        mesh=finer,
        in_specs=(P(dp, None), P(dp, mp), P()),
        out_specs=(P(dp, mp), P(dp, mp), P()),
        check_vma=False,
    )
```
